128 devices in a mesh: tri: 2 (over x_hi), blk: 64 (over y, x_lo, z, core).
Axes of the slice: x: 4 (x_hi: 2, x_lo: 2; x = x_hi * 2 + x_lo), y: 4, z: 4, core: 2. Of those that a mesh axis runs over, the one named last changes fastest.
Arguments:
- layers: float32 [384, 4, 393216], P(('tri', 'blk')), as said below
- tile_mask: int32 [384, 1, 24], P(('tri', 'blk')), may hold values 0 or 1
- depth_order: int32 [384], replicated, may hold values from 0 to 383, as said below
Outputs:
- composite: float32 [4, 393216], P(None, 'blk')
The draws below stay inside these ranges and needn't reach their ends.
Inputs may be any that keep to these rules, and one draw needn't show every extreme that they name: `layers`: in each rank's layer the first three channels lie between 0 and channel 3, and channel 3 lies between 0 and 6 / 384. `depth_order`: A permutation. Ranks are numbered so that device d of the mesh (tri index times 64 plus blk index) holds ranks 3 * d to 3 * d + 2, and these take consecutive positions. The 64 devices of one tri index hold consecutive positions, and for every bit b, the devices of one tri index that agree on all bits of the blk index above bit b hold consecutive positions.
All inputs are finite; a program needn't handle non-finite values. No bound on the sum of `tile_mask` on one device may be relied on, other than what follows from the above.
Results may differ from the reference program's by a relative error of at most 0.00002.
Values sent between devices are 32-bit elements; how exact they have to be, the bound alone decides.
A program may use at most 128 MiB of HBM per device.

```python
import jax
import jax.numpy as jnp
from jax import lax

TILE = 128
RANK_DEV = 3
PIX = 393216
TR = 1
TC = 24
RANKS = 384
N_TRI = 2
N_BLK = 64


def draw_layers(key, part):
    first_key = jax.random.fold_in(key, 11)
    second_key = jax.random.fold_in(key, 12)
    opacity = jax.random.uniform(first_key, (RANKS, 1, PIX), jnp.float32, 0.0, 4.0 / RANKS)
    colours = jax.random.uniform(second_key, (RANKS, 3, PIX), jnp.float32)
    return jnp.concatenate([opacity * colours, opacity], axis=1).astype(jnp.float32)


def draw_depth_order(key, part):
    device_count = N_TRI * N_BLK
    per_group = N_BLK
    levels = per_group.bit_length() - 1
    flip_bits = jax.random.randint(jax.random.fold_in(key, 21), (max(levels, 1), device_count), 0, 2).astype(jnp.int32)
    order_tri = jax.random.permutation(jax.random.fold_in(key, 22), N_TRI).astype(jnp.int32)
    devices_all = jnp.arange(device_count, dtype=jnp.int32)
    within = devices_all % per_group
    group_id = devices_all // per_group
    position = jnp.zeros((device_count,), jnp.int32)
    for section in range(levels):
        parent = devices_all >> section + 1
        flipped = flip_bits[section][parent]
        bit_value = within >> section & 1
        position = position + ((bit_value ^ flipped) << section)
    device_position = order_tri[group_id] * per_group + position
    scores = jax.random.randint(jax.random.fold_in(key, 23), (device_count, RANK_DEV), 0, 1 << 20).astype(jnp.int32)
    scores = scores * RANK_DEV + jnp.arange(RANK_DEV, dtype=jnp.int32)[None, :]
    local_order = jnp.argsort(jnp.argsort(scores, axis=1), axis=1).astype(jnp.int32)
    result = device_position[:, None] * RANK_DEV + local_order
    return result.reshape(RANKS).astype(jnp.int32)


def plant(entries, key, smallest, largest):
    spot = [jax.random.randint(jax.random.fold_in(key, axis), (), 0, length) for axis, length in enumerate(entries.shape)]
    widest = entries.shape.index(max(entries.shape))
    neighbour = spot[:widest] + [(spot[widest] + 1) % entries.shape[widest]] + spot[widest + 1:]
    return entries.at[tuple(spot)].set(smallest).at[tuple(neighbour)].set(largest)


def setup_inputs(seed: int = 0) -> dict:
    seeds = jax.random.split(jax.random.key(seed), 4)
    layers = draw_layers(jax.random.fold_in(seeds[3], 71), 0)
    tile_mask = plant((jax.random.randint(seeds[1], (RANKS, TR, TC), 0, 2) < 1).astype(jnp.int32), jax.random.fold_in(seeds[1], 1), 0, 1)
    depth_order = draw_depth_order(jax.random.fold_in(seeds[3], 71), 0)
    return dict(layers=layers, tile_mask=tile_mask, depth_order=depth_order)


def reference(layers, tile_mask, depth_order):
    ranked = jnp.zeros((RANKS,), jnp.int32).at[depth_order].set(jnp.arange(RANKS, dtype=jnp.int32))

    def advance(carry, which):
        summed, through = carry
        partial_value = lax.dynamic_index_in_dim(layers, which, 0, keepdims=False)
        tile_on = lax.dynamic_index_in_dim(tile_mask, which, 0, keepdims=False).astype(jnp.float32)
        partial_value = (partial_value.reshape(4, TR, TILE, TC, TILE) * tile_on[None, :, None, :, None]).reshape(4, PIX)
        summed = summed + through[None] * partial_value
        through = through * (1.0 - partial_value[3])
        return (summed, through), None

    start = (jnp.zeros((4, PIX), jnp.float32), jnp.ones((PIX,), jnp.float32))
    (summed, through), unused = lax.scan(advance, start, ranked)
    return summed
```

```python
import functools

import jax
import jax.numpy as jnp
from jax import lax
from jax.experimental import pallas as pl
from jax.experimental.pallas import tpu as pltpu
from jax.sharding import PartitionSpec as P

MESH = pl.DeviceIdType.MESH
RANK_DEV = 3
CHANNELS = 4
COLUMN_TILES = 24
BLOCKS = 64
BLOCK_TILES = 48
CHUNK_TILES = 8
CHUNKS = BLOCK_TILES // CHUNK_TILES
ROWS = CHANNELS * CHUNK_TILES


def nearer(depth, left, right):
    return jnp.where(depth[RANK_DEV * left] < depth[RANK_DEV * right], 1.0, 0.0).astype(jnp.float32)


def over(a, b, a_front, b_front):
    through_a = 1.0 - b_front * b[3]
    through_b = 1.0 - a_front * a[3]
    return [through_a * a[ch] + through_b * b[ch] for ch in range(CHANNELS)]


def kernel(layers, tile_mask, depth, out,
           inb, local, from_core, chip, from_pair, pair, from_cross, quad, gathered, outv,
           in_sem, core_send, core_recv, pair_send, pair_recv, cross_send, cross_recv,
           plane_send, plane_recv, out_sem):
    tri = lax.axis_index("tri")
    blk = lax.axis_index("blk")
    core = blk % 2
    z = (blk // 2) % 4
    x = (blk // 8) % 2
    y = blk // 16
    spot = y * 2 + x
    me = tri * BLOCKS + blk
    half = (z % 2 + z // 2) % 2
    item = z // 2

    def device(t, yy, xx, zz, cc):
        return (t, yy * 16 + xx * 8 + zz * 2 + cc)

    core_peer = device(tri, y, x, z, 1 - core)
    pair_peer = device(tri, y, x, z + 1 - 2 * (z % 2), core)
    cross_peer = device(tri, y, x, 3 - z, core)

    def plane_peer(step):
        return (tri + step // 8) % 2, (y + (step // 2) % 4) % 4, (x + step % 2) % 2

    def load_copy(k):
        return pltpu.make_async_copy(
            layers.at[:, :, pl.ds(ROWS * k, ROWS), :], inb.at[k], in_sem.at[k])

    def core_copy(k):
        return pltpu.make_async_remote_copy(
            src_ref=local.at[k, 1 - core], dst_ref=from_core.at[k],
            send_sem=core_send.at[k], recv_sem=core_recv.at[k],
            device_id=core_peer, device_id_type=MESH)

    def pair_copy(k):
        return pltpu.make_async_remote_copy(
            src_ref=chip.at[k, 1 - half], dst_ref=from_pair.at[k],
            send_sem=pair_send.at[k], recv_sem=pair_recv.at[k],
            device_id=pair_peer, device_id_type=MESH)

    def cross_copy(k):
        return pltpu.make_async_remote_copy(
            src_ref=pair.at[k, 1 - item], dst_ref=from_cross.at[k],
            send_sem=cross_send.at[k], recv_sem=cross_recv.at[k],
            device_id=cross_peer, device_id_type=MESH)

    def plane_copy(k, step):
        t, yy, xx = plane_peer(step)
        return pltpu.make_async_remote_copy(
            src_ref=quad.at[k, yy * 2 + xx], dst_ref=gathered.at[k, tri * 8 + spot],
            send_sem=plane_send.at[k, step], recv_sem=plane_recv.at[k, tri * 8 + spot],
            device_id=device(t, yy, xx, z, core), device_id_type=MESH)

    def plane_arrival(k, step):
        t, yy, xx = plane_peer(step)
        source = t * 8 + yy * 2 + xx
        return pltpu.make_async_remote_copy(
            src_ref=quad.at[k, spot], dst_ref=gathered.at[k, source],
            send_sem=plane_send.at[k, step], recv_sem=plane_recv.at[k, source],
            device_id=device(t, yy, xx, z, core), device_id_type=MESH)

    for k in range(CHUNKS):
        load_copy(k).start()

    barrier = pltpu.get_barrier_semaphore()
    for peer in (core_peer, pair_peer, cross_peer):
        pl.semaphore_signal(barrier, inc=1, device_id=peer, device_id_type=MESH)

    @pl.loop(1, 16)
    def _(step):
        t, yy, xx = plane_peer(step)
        pl.semaphore_signal(barrier, inc=1, device_id=device(t, yy, xx, z, core), device_id_type=MESH)

    own = [depth[RANK_DEV * me + r] for r in range(RANK_DEV)]
    front = [[jnp.where(own[j] < own[r], 1.0, 0.0).astype(jnp.float32) for r in range(RANK_DEV)]
             for j in range(RANK_DEV)]

    def flags(peer):
        other = peer[0] * BLOCKS + peer[1]
        return nearer(depth, me, other), nearer(depth, other, me)

    core_flags = flags(core_peer)
    pair_flags = flags(pair_peer)
    cross_flags = flags(cross_peer)

    sub = lax.broadcasted_iota(jnp.int32, (CHUNK_TILES, 128), 0)

    def mask_of(r, group):
        value = jnp.zeros((CHUNK_TILES, 128), jnp.float32)
        for s in range(CHUNK_TILES):
            on = tile_mask[r, 0, CHUNK_TILES * group + s].astype(jnp.float32)
            value = jnp.where(sub == s, on, value)
        return value

    masks = [[mask_of(r, g) for r in range(RANK_DEV)] for g in range(COLUMN_TILES // CHUNK_TILES)]

    def blend_local(k, to_core):
        mask = masks[k % (COLUMN_TILES // CHUNK_TILES)]

        @pl.loop(0, 32)
        def _(n):
            hh, ii, pp = n // 16, (n // 8) % 2, n % 8
            zz = hh + ii * (3 - 2 * hh)
            b = pp * 8 + zz * 2 + to_core

            def plane(r, ch):
                return inb[k, r, b, pl.ds(ch, CHUNK_TILES, stride=CHANNELS), :]

            opacity = [mask[r] * plane(r, 3) for r in range(RANK_DEV)]
            weights = []
            for r in range(RANK_DEV):
                weight = mask[r]
                for j in range(RANK_DEV):
                    if j != r:
                        weight = weight * (1.0 - front[j][r] * opacity[j])
                weights.append(weight)
            for ch in range(CHANNELS):
                total = weights[0] * plane(0, ch)
                for r in range(1, RANK_DEV):
                    total = total + weights[r] * plane(r, ch)
                local[k, to_core, hh, ii, pp, ch] = total

    def blend_chip(k, to_half):
        @pl.loop(0, 16)
        def _(n):
            ii, pp = n // 8, n % 8
            a = [local[k, core, to_half, ii, pp, ch] for ch in range(CHANNELS)]
            b = [from_core[k, to_half, ii, pp, ch] for ch in range(CHANNELS)]
            for ch, value in enumerate(over(a, b, *core_flags)):
                chip[k, to_half, ii, pp, ch] = value

    def blend_pair(k, to_item):
        @pl.loop(0, 8)
        def _(pp):
            a = [chip[k, half, to_item, pp, ch] for ch in range(CHANNELS)]
            b = [from_pair[k, to_item, pp, ch] for ch in range(CHANNELS)]
            for ch, value in enumerate(over(a, b, *pair_flags)):
                pair[k, to_item, pp, ch] = value

    def blend_cross(k):
        @pl.loop(0, 8)
        def _(pp):
            a = [pair[k, item, pp, ch] for ch in range(CHANNELS)]
            b = [from_cross[k, pp, ch] for ch in range(CHANNELS)]
            for ch, value in enumerate(over(a, b, *cross_flags)):
                quad[k, pp, ch] = value

        for ch in range(CHANNELS):
            gathered[k, tri * 8 + spot, ch] = quad[k, spot, ch]

    def quad_device(q):
        return (q // 8) * BLOCKS + (q % 8) * 8

    plane_flags = []
    span = 1
    while span < 16:
        plane_flags.append([
            (nearer(depth, quad_device(q), quad_device(q + span)),
             nearer(depth, quad_device(q + span), quad_device(q)))
            for q in range(0, 16, 2 * span)])
        span *= 2

    def blend_plane(k):
        images = [[gathered[k, q, ch] for ch in range(CHANNELS)] for q in range(16)]
        for level in plane_flags:
            images = [over(images[2 * n], images[2 * n + 1], *level[n]) for n in range(len(level))]
        for ch in range(CHANNELS):
            outv[pl.ds(ROWS * k + ch, CHUNK_TILES, stride=CHANNELS), :] = images[0][ch]

    def first_stage(k):
        load_copy(k).wait()
        blend_local(k, 1 - core)
        if k == 0:
            pl.semaphore_wait(barrier, 18)
        core_copy(k).start()
        blend_local(k, core)

    def second_stage(k):
        core_copy(k).wait_recv()
        blend_chip(k, 1 - half)
        pair_copy(k).start()
        blend_chip(k, half)

    def third_stage(k):
        pair_copy(k).wait_recv()
        blend_pair(k, 1 - item)
        cross_copy(k).start()
        blend_pair(k, item)

    def fourth_stage(k):
        cross_copy(k).wait_recv()
        blend_cross(k)

        @pl.loop(1, 16)
        def _(step):
            plane_copy(k, step).start()

    def last_stage(k):
        @pl.loop(1, 16)
        def _(step):
            plane_arrival(k, step).wait_recv()

        blend_plane(k)

    first_stage(0)
    for k in range(1, CHUNKS):
        first_stage(k)
        second_stage(k - 1)
    second_stage(CHUNKS - 1)
    for k in range(CHUNKS):
        third_stage(k)
        if k >= 1:
            fourth_stage(k - 1)
        if k >= 2:
            last_stage(k - 2)
    fourth_stage(CHUNKS - 1)
    last_stage(CHUNKS - 2)
    last_stage(CHUNKS - 1)
    result = pltpu.make_async_copy(outv, out, out_sem)
    result.start()
    for k in range(CHUNKS):
        core_copy(k).wait_send()
        pair_copy(k).wait_send()
        cross_copy(k).wait_send()

        @pl.loop(1, 16)
        def _(step):
            plane_copy(k, step).wait_send()
    result.wait()


def on_device(layers, tile_mask, depth_order):
    rank_dev, channels, pixels = layers.shape
    tiles = pixels // 128
    rows = layers.reshape(rank_dev, channels, tiles, 128).transpose(0, 2, 1, 3)
    rows = rows.reshape(rank_dev, BLOCKS, BLOCK_TILES * channels, 128)
    image = (CHANNELS, CHUNK_TILES, 128)
    dma = pltpu.SemaphoreType.DMA
    out = pl.pallas_call(
        kernel,
        out_shape=jax.ShapeDtypeStruct((BLOCK_TILES * channels, 128), jnp.float32),
        in_specs=[
            pl.BlockSpec(memory_space=pl.ANY),
            pl.BlockSpec(memory_space=pltpu.SMEM),
            pl.BlockSpec(memory_space=pltpu.SMEM),
        ],
        out_specs=pl.BlockSpec(memory_space=pl.ANY),
        scratch_shapes=[
            pltpu.VMEM((CHUNKS, rank_dev, BLOCKS, ROWS, 128), jnp.float32),
            pltpu.VMEM((CHUNKS, 2, 2, 2, 8) + image, jnp.float32),
            pltpu.VMEM((CHUNKS, 2, 2, 8) + image, jnp.float32),
            pltpu.VMEM((CHUNKS, 2, 2, 8) + image, jnp.float32),
            pltpu.VMEM((CHUNKS, 2, 8) + image, jnp.float32),
            pltpu.VMEM((CHUNKS, 2, 8) + image, jnp.float32),
            pltpu.VMEM((CHUNKS, 8) + image, jnp.float32),
            pltpu.VMEM((CHUNKS, 8) + image, jnp.float32),
            pltpu.VMEM((CHUNKS, 16) + image, jnp.float32),
            pltpu.VMEM((BLOCK_TILES * channels, 128), jnp.float32),
            dma((CHUNKS,)),
            dma((CHUNKS,)), dma((CHUNKS,)),
            dma((CHUNKS,)), dma((CHUNKS,)),
            dma((CHUNKS,)), dma((CHUNKS,)),
            dma((CHUNKS, 16)), dma((CHUNKS, 16)),
            dma,
        ],
        compiler_params=pltpu.CompilerParams(
            collective_id=0, has_side_effects=True, vmem_limit_bytes=60 * 1024 * 1024),
    )(rows, tile_mask, depth_order)
    out = out.reshape(BLOCK_TILES, channels, 128).transpose(1, 0, 2)
    return out.reshape(channels, BLOCK_TILES * 128)


def solution(mesh):
    in_specs = (P(("tri", "blk"), None, None), P(("tri", "blk"), None, None), P())
    out_specs = P(None, "blk")
    return jax.shard_map(
        on_device, mesh=mesh, in_specs=in_specs, out_specs=out_specs, check_vma=False
    )
```

```python
import jax
import jax.numpy as jnp
from jax import lax
from jax.experimental import pallas as pl
from jax.experimental.pallas import tpu as pltpu
from jax.sharding import PartitionSpec as P

MESH = pl.DeviceIdType.MESH
RANK_DEV = 3
CHANNELS = 4
COLUMN_TILES = 24
BLOCKS = 64
BLOCK_TILES = 48
CHUNK_TILES = 8
CHUNKS = BLOCK_TILES // CHUNK_TILES
ROWS = CHANNELS * CHUNK_TILES
SPOTS = 8
UNITS = ((0, 0, 1), (0, 1, 1), (0, 2, 2), (1, 0, 4), (2, 0, 4), (3, 0, 4), (4, 0, 4),
         (5, 0, 2), (5, 2, 1), (5, 3, 1))


def spot_of(y, x):
    return 4 * ((y + x) % 2) + 2 * x + y // 2


def place_of(spot):
    x = (spot // 2) % 2
    return 2 * (spot % 2) + (x + spot // 4) % 2, x


def over(a, b, a_front, b_front):
    through_a = 1.0 - b_front * b[3]
    through_b = 1.0 - a_front * a[3]
    return [through_a * a[ch] + through_b * b[ch] for ch in range(CHANNELS)]


def kernel(layers, mask_in, depth_in, out,
           inb, local, from_core, chip, from_pair, pair, from_cross, quad, gathered, outv,
           tile_mask, depth,
           in_sem, core_send, core_recv, pair_send, pair_recv, cross_send, cross_recv,
           plane_send, plane_recv, small_sem):
    tri = lax.axis_index("tri")
    blk = lax.axis_index("blk")
    core = blk % 2
    z = (blk // 2) % 4
    x = (blk // 8) % 2
    y = blk // 16
    spot = spot_of(y, x)
    me = tri * BLOCKS + blk
    half = (z % 2 + z // 2) % 2
    item = z // 2

    def device(t, yy, xx, zz, cc):
        return (t, yy * 16 + xx * 8 + zz * 2 + cc)

    core_peer = device(tri, y, x, z, 1 - core)
    pair_peer = device(tri, y, x, z + 1 - 2 * (z % 2), core)
    cross_peer = device(tri, y, x, 3 - z, core)

    def load_copy(u, m):
        k, first, _ = UNITS[u]
        low = (m % 2 + m // 2) % 2 * 2 + m % 2
        return pltpu.make_async_copy(
            layers.at[:, :, low, :, pl.ds(ROWS * k, ROWS), :], inb.at[k, m], in_sem.at[u])

    def load_wait(u):
        k, first, count = UNITS[u]
        pltpu.make_async_copy(
            inb.at[k, pl.ds(first, count)], inb.at[k, pl.ds(first, count)], in_sem.at[u]).wait()

    def load_start(u):
        k, first, count = UNITS[u]
        for m in range(first, first + count):
            load_copy(u, m).start()

    def spots(u):
        k, first, count = UNITS[u]
        return k, pl.ds(2 * first, 2 * count)

    def core_copy(u):
        k, part = spots(u)
        return pltpu.make_async_remote_copy(
            src_ref=local.at[k, 1 - core, :, :, part], dst_ref=from_core.at[k, :, :, part],
            send_sem=core_send.at[u], recv_sem=core_recv.at[u],
            device_id=core_peer, device_id_type=MESH)

    def pair_copy(u):
        k, part = spots(u)
        return pltpu.make_async_remote_copy(
            src_ref=chip.at[k, 1 - half, :, part], dst_ref=from_pair.at[k, :, part],
            send_sem=pair_send.at[u], recv_sem=pair_recv.at[u],
            device_id=pair_peer, device_id_type=MESH)

    def cross_copy(u):
        k, part = spots(u)
        return pltpu.make_async_remote_copy(
            src_ref=pair.at[k, 1 - item, part], dst_ref=from_cross.at[k, part],
            send_sem=cross_send.at[u], recv_sem=cross_recv.at[u],
            device_id=cross_peer, device_id_type=MESH)

    def plane_copy(k, t, other):
        yy, xx = place_of(other)
        return pltpu.make_async_remote_copy(
            src_ref=quad.at[k, other], dst_ref=gathered.at[k, tri * SPOTS + spot],
            send_sem=plane_send.at[k], recv_sem=plane_recv.at[k],
            device_id=device(t, yy, xx, z, core), device_id_type=MESH)

    def plane_all(k):
        return pltpu.make_async_remote_copy(
            src_ref=gathered.at[k, pl.ds(0, 2 * SPOTS - 1)],
            dst_ref=gathered.at[k, pl.ds(0, 2 * SPOTS - 1)],
            send_sem=plane_send.at[k], recv_sem=plane_recv.at[k],
            device_id=core_peer, device_id_type=MESH)

    mask_copy = pltpu.make_async_copy(mask_in, tile_mask, small_sem.at[0])
    depth_copy = pltpu.make_async_copy(depth_in, depth, small_sem.at[1])
    mask_copy.start()
    depth_copy.start()
    load_start(0)
    load_start(1)

    barrier = pltpu.get_barrier_semaphore()
    for peer in (core_peer, pair_peer, cross_peer):
        pl.semaphore_signal(barrier, inc=1, device_id=peer, device_id_type=MESH)
    for step in range(1, 2 * SPOTS):
        t = (tri + step // SPOTS) % 2
        yy, xx = place_of((spot + step) % SPOTS)
        pl.semaphore_signal(barrier, inc=1, device_id=device(t, yy, xx, z, core), device_id_type=MESH)

    for u in range(2, len(UNITS)):
        load_start(u)
    mask_copy.wait()
    depth_copy.wait()

    def nearer(left, right):
        return jnp.where(
            depth[RANK_DEV * left] < depth[RANK_DEV * right], 1.0, 0.0).astype(jnp.float32)

    own = [depth[RANK_DEV * me + r] for r in range(RANK_DEV)]
    front = [[jnp.where(own[j] < own[r], 1.0, 0.0).astype(jnp.float32) for r in range(RANK_DEV)]
             for j in range(RANK_DEV)]

    def flags(peer):
        other = peer[0] * BLOCKS + peer[1]
        return nearer(me, other), nearer(other, me)

    core_flags = flags(core_peer)
    pair_flags = flags(pair_peer)
    cross_flags = flags(cross_peer)

    def quad_device(q):
        yy, xx = (q // 2) % 4, q % 2
        return (q // 8) * BLOCKS + yy * 16 + xx * 8

    plane_flags = []
    span = 1
    while span < 2 * SPOTS:
        plane_flags.append([
            (nearer(quad_device(q), quad_device(q + span)),
             nearer(quad_device(q + span), quad_device(q)))
            for q in range(0, 2 * SPOTS, 2 * span)])
        span *= 2

    sub = lax.broadcasted_iota(jnp.int32, (CHUNK_TILES, 128), 0)

    def mask_of(r, group):
        value = jnp.zeros((CHUNK_TILES, 128), jnp.float32)
        for s in range(CHUNK_TILES):
            on = tile_mask[r, 0, CHUNK_TILES * group + s].astype(jnp.float32)
            value = jnp.where(sub == s, on, value)
        return value

    masks = [[mask_of(r, g) for r in range(RANK_DEV)] for g in range(COLUMN_TILES // CHUNK_TILES)]

    def blend_local(u, to_core):
        k, first, count = UNITS[u]
        mask = masks[k % (COLUMN_TILES // CHUNK_TILES)]
        for hh in range(2):
            for ii in range(2):
                block = (hh + ii * (3 - 2 * hh)) * 2 + to_core

                @pl.loop(2 * first, 2 * (first + count), unroll=2)
                def _(o):
                    def plane(r, ch):
                        return inb[k, o // 2, r, o % 2, block,
                                   pl.ds(ch, CHUNK_TILES, stride=CHANNELS), :]

                    opacity = [mask[r] * plane(r, 3) for r in range(RANK_DEV)]
                    weights = []
                    for r in range(RANK_DEV):
                        weight = mask[r]
                        for j in range(RANK_DEV):
                            if j != r:
                                weight = weight * (1.0 - front[j][r] * opacity[j])
                        weights.append(weight)
                    for ch in range(CHANNELS):
                        total = weights[0] * plane(0, ch)
                        for r in range(1, RANK_DEV):
                            total = total + weights[r] * plane(r, ch)
                        local[k, to_core, hh, ii, o, ch] = total

    def blend_chip(u, to_half):
        k, first, count = UNITS[u]
        for ii in range(2):
            @pl.loop(2 * first, 2 * (first + count), unroll=2)
            def _(o):
                a = [local[k, core, to_half, ii, o, ch] for ch in range(CHANNELS)]
                b = [from_core[k, to_half, ii, o, ch] for ch in range(CHANNELS)]
                for ch, value in enumerate(over(a, b, *core_flags)):
                    chip[k, to_half, ii, o, ch] = value

    def blend_pair(u, to_item):
        k, first, count = UNITS[u]

        @pl.loop(2 * first, 2 * (first + count), unroll=2)
        def _(o):
            a = [chip[k, half, to_item, o, ch] for ch in range(CHANNELS)]
            b = [from_pair[k, to_item, o, ch] for ch in range(CHANNELS)]
            for ch, value in enumerate(over(a, b, *pair_flags)):
                pair[k, to_item, o, ch] = value

    def blend_cross(u):
        k, first, count = UNITS[u]

        @pl.loop(2 * first, 2 * (first + count), unroll=2)
        def _(o):
            a = [pair[k, item, o, ch] for ch in range(CHANNELS)]
            b = [from_cross[k, o, ch] for ch in range(CHANNELS)]
            for ch, value in enumerate(over(a, b, *cross_flags)):
                quad[k, o, ch] = value

    def blend_plane(k):
        for ch in range(CHANNELS):
            gathered[k, tri * SPOTS + spot, ch] = quad[k, spot, ch]
        images = []
        for q in range(2 * SPOTS):
            slot = (q // SPOTS) * SPOTS + spot_of((q // 2) % 4, q % 2)
            images.append([gathered[k, slot, ch] for ch in range(CHANNELS)])
        for level in plane_flags:
            images = [over(images[2 * n], images[2 * n + 1], *level[n]) for n in range(len(level))]
        for ch in range(CHANNELS):
            outv[pl.ds(ROWS * k + ch, CHUNK_TILES, stride=CHANNELS), :] = images[0][ch]

    def first_stage(u):
        with jax.named_scope(f"w_load{u}"):
            load_wait(u)
        with jax.named_scope(f"c_local{u}"):
            blend_local(u, 1 - core)
        if u == 0:
            with jax.named_scope("w_barrier"):
                pl.semaphore_wait(barrier, 18)
        core_copy(u).start()
        with jax.named_scope(f"c_own{u}"):
            blend_local(u, core)

    def second_stage(u):
        with jax.named_scope(f"w_core{u}"):
            core_copy(u).wait_recv()
        with jax.named_scope(f"c_chip{u}"):
            blend_chip(u, 1 - half)
        pair_copy(u).start()
        with jax.named_scope(f"c_chipown{u}"):
            blend_chip(u, half)

    def third_stage(u):
        with jax.named_scope(f"w_pair{u}"):
            pair_copy(u).wait_recv()
        with jax.named_scope(f"c_pair{u}"):
            blend_pair(u, 1 - item)
        cross_copy(u).start()
        with jax.named_scope(f"c_pairown{u}"):
            blend_pair(u, item)

    def fourth_stage(u):
        k, first, count = UNITS[u]
        with jax.named_scope(f"w_cross{u}"):
            cross_copy(u).wait_recv()
        with jax.named_scope(f"c_cross{u}"):
            blend_cross(u)
        with jax.named_scope(f"s_plane{u}"):
            for step in range(4 * count):
                t = (tri + 1 + step // (2 * count)) % 2
                other = 2 * first + (spot + step) % (2 * count)

                @pl.when((t != tri) | (other != spot))
                def _():
                    plane_copy(k, t, other).start()

    def last_stage(k):
        with jax.named_scope(f"w_plane{k}"):
            plane_all(k).wait_recv()
        with jax.named_scope(f"c_plane{k}"):
            blend_plane(k)

    first_stage(0)
    for u in range(1, len(UNITS)):
        first_stage(u)
        second_stage(u - 1)
    second_stage(len(UNITS) - 1)
    for u in range(len(UNITS)):
        third_stage(u)
        if u >= 1:
            fourth_stage(u - 1)
    fourth_stage(len(UNITS) - 1)
    for k in range(CHUNKS - 1):
        last_stage(k)
    with jax.named_scope("w_sends"):
        for u in range(len(UNITS)):
            core_copy(u).wait_send()
            pair_copy(u).wait_send()
            cross_copy(u).wait_send()
        for k in range(CHUNKS):
            plane_all(k).wait_send()
    last_stage(CHUNKS - 1)
    with jax.named_scope("w_out"):
        result = pltpu.make_async_copy(outv, out, small_sem.at[0])
        result.start()
        result.wait()


def on_device(layers, tile_mask, depth_order):
    rank_dev, channels, pixels = layers.shape
    tiles = pixels // 128
    rows = layers.reshape(rank_dev, channels, tiles, 128).transpose(0, 2, 1, 3)
    rows = rows.reshape(rank_dev, 2, 4, 8, BLOCK_TILES * channels, 128)
    image = (CHANNELS, CHUNK_TILES, 128)
    units = len(UNITS)
    dma = pltpu.SemaphoreType.DMA
    out = pl.pallas_call(
        kernel,
        out_shape=jax.ShapeDtypeStruct((BLOCK_TILES * channels, 128), jnp.float32),
        in_specs=[pl.BlockSpec(memory_space=pltpu.HBM)] * 3,
        out_specs=pl.BlockSpec(memory_space=pl.ANY),
        scratch_shapes=[
            pltpu.VMEM((CHUNKS, 4, rank_dev, 2, 8, ROWS, 128), jnp.float32),
            pltpu.VMEM((CHUNKS, 2, 2, 2, SPOTS) + image, jnp.float32),
            pltpu.VMEM((CHUNKS, 2, 2, SPOTS) + image, jnp.float32),
            pltpu.VMEM((CHUNKS, 2, 2, SPOTS) + image, jnp.float32),
            pltpu.VMEM((CHUNKS, 2, SPOTS) + image, jnp.float32),
            pltpu.VMEM((CHUNKS, 2, SPOTS) + image, jnp.float32),
            pltpu.VMEM((CHUNKS, SPOTS) + image, jnp.float32),
            pltpu.VMEM((CHUNKS, SPOTS) + image, jnp.float32),
            pltpu.VMEM((CHUNKS, 2 * SPOTS) + image, jnp.float32),
            pltpu.VMEM((BLOCK_TILES * channels, 128), jnp.float32),
            pltpu.SMEM(tile_mask.shape, jnp.int32),
            pltpu.SMEM(depth_order.shape, jnp.int32),
            dma((units,)),
            dma((units,)), dma((units,)),
            dma((units,)), dma((units,)),
            dma((units,)), dma((units,)),
            dma((CHUNKS,)), dma((CHUNKS,)),
            dma((2,)),
        ],
        compiler_params=pltpu.CompilerParams(
            collective_id=0, has_side_effects=True, vmem_limit_bytes=60 * 1024 * 1024),
    )(rows, tile_mask, depth_order)
    out = out.reshape(BLOCK_TILES, channels, 128).transpose(1, 0, 2)
    return out.reshape(channels, BLOCK_TILES * 128)


def solution(mesh):
    in_specs = (P(("tri", "blk"), None, None), P(("tri", "blk"), None, None), P())
    out_specs = P(None, "blk")
    return jax.shard_map(
        on_device, mesh=mesh, in_specs=in_specs, out_specs=out_specs, check_vma=False
    )
```

```python
import jax
import jax.numpy as jnp
from jax import lax
from jax.experimental import pallas as pl
from jax.experimental.pallas import tpu as pltpu
from jax.sharding import PartitionSpec as P

MESH = pl.DeviceIdType.MESH
RANK_DEV = 3
CHANNELS = 4
COLUMN_TILES = 24
BLOCKS = 64
BLOCK_TILES = 48
CHUNK_TILES = 8
CHUNKS = BLOCK_TILES // CHUNK_TILES
ROWS = CHANNELS * CHUNK_TILES
SPOTS = 8
UNITS = (
    (0, 0, 1, 'P'),
    (0, 1, 1, 'P'),
    (0, 2, 1, 'P'),
    (0, 3, 1, 'P'),
    (1, 0, 4, 'P'),
    (2, 0, 2, 'P'),
    (2, 2, 1, 'T'),
    (2, 3, 1, 'T'),
    (3, 0, 2, 'T'),
    (3, 2, 2, 'T'),
    (4, 0, 4, 'T'),
    (5, 0, 1, 'T'),
    (5, 1, 1, 'T'),
    (5, 2, 1, 'T'),
    (5, 3, 1, 'T'),
)
LOADS = (3, 6, 1, 10, 2, 4, 5, 9, 8, 0, 14, 7, 11, 13, 12)
FAR = (5,)
PLAN = (
    ('L', 3), ('L', 6), ('L', 1), ('L', 10), ('C', 3), ('S', 3), ('C', 6), ('S', 6), ('C', 1),
    ('S', 1), ('L', 2), ('L', 4), ('C', 10), ('S', 10), ('C', 2), ('S', 2), ('L', 5), ('L', 9),
    ('L', 8), ('A', 3), ('A', 6), ('C', 4), ('S', 4), ('C', 5), ('L', 0), ('L', 14), ('C', 9),
    ('L', 7), ('L', 11), ('C', 8), ('A', 1), ('L', 13), ('C', 0), ('L', 12), ('C', 14), ('C', 7),
    ('S', 9), ('C', 11), ('C', 13), ('A', 2), ('C', 12), ('B', 6), ('A', 10), ('S', 8), ('B', 3),
    ('B', 1), ('S', 5), ('S', 14), ('A', 4), ('D', 6), ('A', 9), ('B', 10), ('B', 2), ('S', 7),
    ('A', 5), ('B', 9), ('A', 8), ('A', 14), ('S', 11), ('S', 0), ('D', 10), ('S', 13), ('B', 4),
    ('S', 12), ('D', 9), ('B', 8), ('A', 7), ('B', 14), ('B', 5), ('A', 0), ('A', 11), ('G', 4),
    ('D', 8), ('B', 7), ('A', 13), ('D', 14), ('B', 11), ('G', 1), ('A', 12), ('D', 7), ('B', 13),
    ('B', 0), ('F', 4), ('D', 11), ('B', 12), ('G', 3), ('D', 13), ('F', 1), ('D', 12), ('G', 2),
    ('G', 0), ('F', 3), ('F', 2), ('F', 0), ('F', 5),
)


def spot_of(y, x):
    return 4 * ((y + x) % 2) + 2 * x + y // 2


def place_of(spot):
    x = (spot // 2) % 2
    return 2 * (spot % 2) + (x + spot // 4) % 2, x


def over(a, b, a_front, b_front):
    through_a = 1.0 - b_front * b[3]
    through_b = 1.0 - a_front * a[3]
    return [through_a * a[ch] + through_b * b[ch] for ch in range(CHANNELS)]


def kernel(layers, mask_in, depth_in, out,
           inb, local, from_core, chip, from_pair, pair, from_cross, from_skip, gap, from_gap,
           merged, from_merged, quad, gathered, group, from_group, outv, tile_mask, depth,
           in_sem, core_send, core_recv, first_send, first_recv, second_send, second_recv,
           third_send, third_recv, plane_send, plane_recv, group_send, group_recv, small_sem):
    tri = lax.axis_index("tri")
    blk = lax.axis_index("blk")
    core = blk % 2
    z = (blk // 2) % 4
    x = (blk // 8) % 2
    y = blk // 16
    spot = spot_of(y, x)
    me = tri * BLOCKS + blk
    half = (z % 2 + z // 2) % 2
    item = z // 2

    def device(t, yy, xx, zz, cc):
        return (t, yy * 16 + xx * 8 + zz * 2 + cc)

    core_peer = device(tri, y, x, z, 1 - core)
    pair_peer = device(tri, y, x, z + 1 - 2 * (z % 2), core)
    cross_peer = device(tri, y, x, 3 - z, core)
    skew_peer = device(tri, y, x, (z + 2) % 4, core)
    tri_peer = device(1 - tri, y, x, z, core)

    def load_copy(u, m):
        k, first, _, _ = UNITS[u]
        low = (m % 2 + m // 2) % 2 * 2 + m % 2
        return pltpu.make_async_copy(
            layers.at[:, :, low, :, pl.ds(ROWS * k, ROWS), :], inb.at[k, m], in_sem.at[u])

    def load_wait(u):
        k, first, count, _ = UNITS[u]
        pltpu.make_async_copy(
            inb.at[k, pl.ds(first, count)], inb.at[k, pl.ds(first, count)], in_sem.at[u]).wait()

    def load_start(u):
        k, first, count, _ = UNITS[u]
        for m in range(first, first + count):
            load_copy(u, m).start()

    def spots(u):
        k, first, count, _ = UNITS[u]
        return k, pl.ds(2 * first, 2 * count)

    def core_copy(u):
        k, part = spots(u)
        return pltpu.make_async_remote_copy(
            src_ref=local.at[k, 1 - core, :, :, part], dst_ref=from_core.at[k, :, :, part],
            send_sem=core_send.at[u], recv_sem=core_recv.at[u],
            device_id=core_peer, device_id_type=MESH)

    def remote(src, dst, send_sem, recv_sem, peer):
        return pltpu.make_async_remote_copy(
            src_ref=src, dst_ref=dst, send_sem=send_sem, recv_sem=recv_sem,
            device_id=peer, device_id_type=MESH)

    def first_copy(u):
        k, part = spots(u)
        if UNITS[u][3] == "P":
            return remote(chip.at[k, 1 - half, :, part], from_pair.at[k, :, part],
                          first_send.at[u], first_recv.at[u], pair_peer)
        return remote(chip.at[k, :, 1 - item, part], from_skip.at[k, :, part],
                      first_send.at[u], first_recv.at[u], cross_peer)

    def second_copy(u):
        k, part = spots(u)
        if UNITS[u][3] == "P":
            return remote(pair.at[k, 1 - item, part], from_cross.at[k, part],
                          second_send.at[u], second_recv.at[u], cross_peer)
        return remote(gap.at[k, part], from_gap.at[k, part],
                      second_send.at[u], second_recv.at[u], pair_peer)

    def third_copy(u):
        k, part = spots(u)
        return remote(merged.at[k, part], from_merged.at[k, part],
                      third_send.at[u], third_recv.at[u], pair_peer)

    def group_copy(k):
        return remote(group.at[k], from_group.at[k], group_send.at[k], group_recv.at[k], tri_peer)

    def plane_copy(k, t, other):
        yy, xx = place_of(other)
        return pltpu.make_async_remote_copy(
            src_ref=quad.at[k, other], dst_ref=gathered.at[k, tri * SPOTS + spot],
            send_sem=plane_send.at[k], recv_sem=plane_recv.at[k],
            device_id=device(t, yy, xx, z, core), device_id_type=MESH)

    def plane_all(k):
        count = 2 * SPOTS - 1 if k in FAR else SPOTS - 1
        return remote(gathered.at[k, pl.ds(0, count)], gathered.at[k, pl.ds(0, count)],
                      plane_send.at[k], plane_recv.at[k], core_peer)

    mask_copy = pltpu.make_async_copy(mask_in, tile_mask, small_sem.at[0])
    depth_copy = pltpu.make_async_copy(depth_in, depth, small_sem.at[1])
    mask_copy.start()
    depth_copy.start()
    for u in LOADS[:2]:
        load_start(u)

    barrier = pltpu.get_barrier_semaphore()
    for peer in (core_peer, pair_peer, cross_peer):
        pl.semaphore_signal(barrier, inc=1, device_id=peer, device_id_type=MESH)
    for step in range(1, 2 * SPOTS):
        t = (tri + step // SPOTS) % 2
        yy, xx = place_of((spot + step) % SPOTS)
        pl.semaphore_signal(barrier, inc=1, device_id=device(t, yy, xx, z, core), device_id_type=MESH)

    for u in LOADS[2:]:
        load_start(u)
    mask_copy.wait()
    depth_copy.wait()

    def nearer(left, right):
        return jnp.where(
            depth[RANK_DEV * left] < depth[RANK_DEV * right], 1.0, 0.0).astype(jnp.float32)

    own = [depth[RANK_DEV * me + r] for r in range(RANK_DEV)]
    front = [[jnp.where(own[j] < own[r], 1.0, 0.0).astype(jnp.float32) for r in range(RANK_DEV)]
             for j in range(RANK_DEV)]

    def number(peer):
        return peer[0] * BLOCKS + peer[1]

    def flags(peer):
        return nearer(me, number(peer)), nearer(number(peer), me)

    core_flags = flags(core_peer)
    pair_flags = flags(pair_peer)
    cross_flags = flags(cross_peer)
    group_flags = flags(tri_peer)

    chips = {"w": me, "v": number(cross_peer), "p": number(pair_peer), "q": number(skew_peer)}
    f = {a + b: nearer(chips[a], chips[b]) for a in chips for b in chips if a != b}
    w_between = f["pw"] * f["wq"] + f["qw"] * f["wp"]
    v_between = f["pv"] * f["vq"] + f["qv"] * f["vp"]
    w_ahead = f["wp"] * f["wq"]
    v_ahead = f["vp"] * f["vq"]

    def quad_device(q):
        return (q // 8) * BLOCKS + (q // 2) % 4 * 16 + q % 2 * 8

    def tree_flags(leaves, base):
        levels = []
        span = 1
        while span < leaves:
            levels.append([
                (nearer(base + quad_device(q), base + quad_device(q + span)),
                 nearer(base + quad_device(q + span), base + quad_device(q)))
                for q in range(0, leaves, 2 * span)])
            span *= 2
        return levels

    far_flags = tree_flags(2 * SPOTS, 0) if FAR else None
    near_flags = tree_flags(SPOTS, tri * BLOCKS)

    sub = lax.broadcasted_iota(jnp.int32, (CHUNK_TILES, 128), 0)

    def mask_of(r, group):
        value = jnp.zeros((CHUNK_TILES, 128), jnp.float32)
        for s in range(CHUNK_TILES):
            on = tile_mask[r, 0, CHUNK_TILES * group + s].astype(jnp.float32)
            value = jnp.where(sub == s, on, value)
        return value

    masks = [[mask_of(r, g) for r in range(RANK_DEV)] for g in range(COLUMN_TILES // CHUNK_TILES)]

    def span_of(u):
        k, first, count, _ = UNITS[u]
        return 2 * first, 2 * (first + count)

    def blend_local(u, to_core):
        k = UNITS[u][0]
        mask = masks[k % (COLUMN_TILES // CHUNK_TILES)]
        first, stop = span_of(u)
        size = stop - first

        @pl.loop(0, 4 * size, unroll=2)
        def _(n):
            hh, ii, o = n // (2 * size), n // size % 2, first + n % size
            block = (hh + ii * (3 - 2 * hh)) * 2 + to_core

            def plane(r, ch):
                return inb[k, o // 2, r, o % 2, block,
                           pl.ds(ch, CHUNK_TILES, stride=CHANNELS), :]

            opacity = [mask[r] * plane(r, 3) for r in range(RANK_DEV)]
            weights = []
            for r in range(RANK_DEV):
                weight = mask[r]
                for j in range(RANK_DEV):
                    if j != r:
                        weight = weight * (1.0 - front[j][r] * opacity[j])
                weights.append(weight)
            for ch in range(CHANNELS):
                total = weights[0] * plane(0, ch)
                for r in range(1, RANK_DEV):
                    total = total + weights[r] * plane(r, ch)
                local[k, to_core, hh, ii, o, ch] = total

    def planes(ref, *index):
        return [ref[index + (ch,)] for ch in range(CHANNELS)]

    def blend_chip(u, sent):
        k, _, _, kind = UNITS[u]
        first, stop = span_of(u)
        size = stop - first

        @pl.loop(0, 2 * size, unroll=2)
        def _(n):
            o = first + n % size
            if kind == "P":
                hh, ii = 1 - half if sent else half, n // size
            else:
                hh, ii = n // size, 1 - item if sent else item
            a = planes(local, k, core, hh, ii, o)
            b = planes(from_core, k, hh, ii, o)
            for ch, value in enumerate(over(a, b, *core_flags)):
                chip[k, hh, ii, o, ch] = value

    def blend_pair(u, to_item):
        k = UNITS[u][0]

        @pl.loop(*span_of(u), unroll=2)
        def _(o):
            a = planes(chip, k, half, to_item, o)
            b = planes(from_pair, k, to_item, o)
            for ch, value in enumerate(over(a, b, *pair_flags)):
                pair[k, to_item, o, ch] = value

    def blend_cross(u):
        k = UNITS[u][0]

        @pl.loop(*span_of(u), unroll=2)
        def _(o):
            a = planes(pair, k, item, o)
            b = planes(from_cross, k, o)
            for ch, value in enumerate(over(a, b, *cross_flags)):
                quad[k, o, ch] = value

    def blend_gap(u):
        k = UNITS[u][0]

        @pl.loop(*span_of(u), unroll=2)
        def _(o):
            gap[k, o] = ((1.0 - w_between * chip[k, half, item, o, 3])
                         * (1.0 - v_between * from_skip[k, half, o, 3]))

    def blend_merged(u):
        k = UNITS[u][0]

        @pl.loop(*span_of(u), unroll=2)
        def _(o):
            w = planes(chip, k, 1 - half, item, o)
            v = planes(from_skip, k, 1 - half, o)
            g = from_gap[k, o]
            weight_w = f["wv"] + f["vw"] * ((1.0 - v[3]) * g)
            weight_v = f["vw"] + f["wv"] * ((1.0 - w[3]) * g)
            for ch in range(3):
                merged[k, o, ch] = weight_w * w[ch] + weight_v * v[ch]
            merged[k, o, 3] = w[3]
            merged[k, o, 4] = v[3]

    def blend_skip(u):
        k = UNITS[u][0]

        @pl.loop(*span_of(u), unroll=2)
        def _(o):
            w = planes(chip, k, half, item, o)
            v = planes(from_skip, k, half, o)
            g = gap[k, o]
            p = from_merged[k, o, 3]
            q = from_merged[k, o, 4]
            m = [from_merged[k, o, ch] for ch in range(3)]
            m.append((f["pq"] + f["qp"] * ((1.0 - q) * g)) * p
                     + (f["qp"] + f["pq"] * ((1.0 - p) * g)) * q)
            weight_w = (1.0 - f["vw"] * v[3]) * (1.0 - f["pw"] * p) * (1.0 - f["qw"] * q)
            weight_v = (1.0 - f["wv"] * w[3]) * (1.0 - f["pv"] * p) * (1.0 - f["qv"] * q)
            weight_m = (1.0 - w_ahead * w[3]) * (1.0 - v_ahead * v[3])
            for ch in range(CHANNELS):
                quad[k, o, ch] = weight_w * w[ch] + weight_v * v[ch] + weight_m * m[ch]

    def blend_tree(k, leaves, base, levels):
        for ch in range(CHANNELS):
            gathered[k, tri * SPOTS + spot, ch] = quad[k, spot, ch]
        images = []
        for q in range(leaves):
            slot = base + (q // SPOTS) * SPOTS + spot_of((q // 2) % 4, q % 2)
            images.append(planes(gathered, k, slot))
        for level in levels:
            images = [over(images[2 * n], images[2 * n + 1], *level[n]) for n in range(len(level))]
        return images[0]

    def put(k, image):
        for ch in range(CHANNELS):
            outv[pl.ds(ROWS * k + ch, CHUNK_TILES, stride=CHANNELS), :] = image[ch]

    def stage_load(u):
        with jax.named_scope(f"L_wait{u}"):
            load_wait(u)
        with jax.named_scope(f"L_send{u}"):
            blend_local(u, 1 - core)
        if u == LOADS[0]:
            with jax.named_scope("w_barrier"):
                pl.semaphore_wait(barrier, 18)
        core_copy(u).start()
        with jax.named_scope(f"L_own{u}"):
            blend_local(u, core)

    def stage_chip(u):
        with jax.named_scope(f"C_wait{u}"):
            core_copy(u).wait_recv()
        with jax.named_scope(f"C_run{u}"):
            blend_chip(u, True)

    def stage_send(u):
        first_copy(u).start()
        with jax.named_scope(f"S_run{u}"):
            blend_chip(u, False)

    def stage_first(u):
        with jax.named_scope(f"A_wait{u}"):
            first_copy(u).wait_recv()
        if UNITS[u][3] == "P":
            with jax.named_scope(f"A_run{u}"):
                blend_pair(u, 1 - item)
            second_copy(u).start()
            blend_pair(u, item)
        else:
            with jax.named_scope(f"A_run{u}"):
                blend_gap(u)
            second_copy(u).start()

    def send_planes(u):
        k, first, count, _ = UNITS[u]
        for step in range(4 * count if k in FAR else 2 * count):
            other = 2 * first + (spot + step) % (2 * count)
            t = (tri + 1 + step // (2 * count)) % 2 if k in FAR else tri

            @pl.when((t != tri) | (other != spot))
            def _():
                plane_copy(k, t, other).start()

    def stage_second(u):
        with jax.named_scope(f"B_wait{u}"):
            second_copy(u).wait_recv()
        if UNITS[u][3] == "P":
            with jax.named_scope(f"B_run{u}"):
                blend_cross(u)
                send_planes(u)
        else:
            with jax.named_scope(f"B_run{u}"):
                blend_merged(u)
            third_copy(u).start()

    def stage_third(u):
        with jax.named_scope(f"D_wait{u}"):
            third_copy(u).wait_recv()
        with jax.named_scope(f"D_run{u}"):
            blend_skip(u)
            send_planes(u)

    def stage_group(k):
        with jax.named_scope(f"G_wait{k}"):
            plane_all(k).wait_recv()
        with jax.named_scope(f"G_run{k}"):
            for ch, value in enumerate(blend_tree(k, SPOTS, tri * SPOTS, near_flags)):
                group[k, ch] = value
        group_copy(k).start()

    def stage_out(k):
        if k in FAR:
            with jax.named_scope(f"F_wait{k}"):
                plane_all(k).wait_recv()
            with jax.named_scope(f"F_run{k}"):
                put(k, blend_tree(k, 2 * SPOTS, 0, far_flags))
        else:
            with jax.named_scope(f"F_wait{k}"):
                group_copy(k).wait_recv()
            with jax.named_scope(f"F_run{k}"):
                put(k, over(planes(group, k), planes(from_group, k), *group_flags))

    stages = {"L": stage_load, "C": stage_chip, "S": stage_send, "A": stage_first,
              "B": stage_second, "D": stage_third, "G": stage_group, "F": stage_out}
    for name, which in PLAN:
        stages[name](which)
    with jax.named_scope("w_sends"):
        for u in range(len(UNITS)):
            core_copy(u).wait_send()
            first_copy(u).wait_send()
            second_copy(u).wait_send()
            if UNITS[u][3] == "T":
                third_copy(u).wait_send()
        for k in range(CHUNKS):
            plane_all(k).wait_send()
            if k not in FAR:
                group_copy(k).wait_send()
    with jax.named_scope("w_out"):
        result = pltpu.make_async_copy(outv, out, small_sem.at[0])
        result.start()
        result.wait()


def on_device(layers, tile_mask, depth_order):
    rank_dev, channels, pixels = layers.shape
    tiles = pixels // 128
    rows = layers.reshape(rank_dev, channels, tiles, 128).transpose(0, 2, 1, 3)
    rows = rows.reshape(rank_dev, 2, 4, 8, BLOCK_TILES * channels, 128)
    plane = (CHUNK_TILES, 128)
    image = (CHANNELS,) + plane
    units = len(UNITS)
    dma = pltpu.SemaphoreType.DMA
    out = pl.pallas_call(
        kernel,
        out_shape=jax.ShapeDtypeStruct((BLOCK_TILES * channels, 128), jnp.float32),
        in_specs=[pl.BlockSpec(memory_space=pltpu.HBM)] * 3,
        out_specs=pl.BlockSpec(memory_space=pl.ANY),
        scratch_shapes=[
            pltpu.VMEM((CHUNKS, 4, rank_dev, 2, 8, ROWS, 128), jnp.float32),
            pltpu.VMEM((CHUNKS, 2, 2, 2, SPOTS) + image, jnp.float32),
            pltpu.VMEM((CHUNKS, 2, 2, SPOTS) + image, jnp.float32),
            pltpu.VMEM((CHUNKS, 2, 2, SPOTS) + image, jnp.float32),
            pltpu.VMEM((CHUNKS, 2, SPOTS) + image, jnp.float32),
            pltpu.VMEM((CHUNKS, 2, SPOTS) + image, jnp.float32),
            pltpu.VMEM((CHUNKS, SPOTS) + image, jnp.float32),
            pltpu.VMEM((CHUNKS, 2, SPOTS) + image, jnp.float32),
            pltpu.VMEM((CHUNKS, SPOTS) + plane, jnp.float32),
            pltpu.VMEM((CHUNKS, SPOTS) + plane, jnp.float32),
            pltpu.VMEM((CHUNKS, SPOTS, 5) + plane, jnp.float32),
            pltpu.VMEM((CHUNKS, SPOTS, 5) + plane, jnp.float32),
            pltpu.VMEM((CHUNKS, SPOTS) + image, jnp.float32),
            pltpu.VMEM((CHUNKS, 2 * SPOTS) + image, jnp.float32),
            pltpu.VMEM((CHUNKS,) + image, jnp.float32),
            pltpu.VMEM((CHUNKS,) + image, jnp.float32),
            pltpu.VMEM((BLOCK_TILES * channels, 128), jnp.float32),
            pltpu.SMEM(tile_mask.shape, jnp.int32),
            pltpu.SMEM(depth_order.shape, jnp.int32),
            dma((units,)),
            dma((units,)), dma((units,)),
            dma((units,)), dma((units,)),
            dma((units,)), dma((units,)),
            dma((units,)), dma((units,)),
            dma((CHUNKS,)), dma((CHUNKS,)),
            dma((CHUNKS,)), dma((CHUNKS,)),
            dma((2,)),
        ],
        compiler_params=pltpu.CompilerParams(
            collective_id=0, has_side_effects=True, vmem_limit_bytes=60 * 1024 * 1024),
    )(rows, tile_mask, depth_order)
    out = out.reshape(BLOCK_TILES, channels, 128).transpose(1, 0, 2)
    return out.reshape(channels, BLOCK_TILES * 128)


def solution(mesh):
    in_specs = (P(("tri", "blk"), None, None), P(("tri", "blk"), None, None), P())
    out_specs = P(None, "blk")
    return jax.shard_map(
        on_device, mesh=mesh, in_specs=in_specs, out_specs=out_specs, check_vma=False
    )
```

```python
import jax
import jax.numpy as jnp
from jax import lax
from jax.experimental import pallas as pl
from jax.experimental.pallas import tpu as pltpu
from jax.sharding import PartitionSpec as P

MESH = pl.DeviceIdType.MESH
RANK_DEV = 3
CHANNELS = 4
COLUMN_TILES = 24
BLOCKS = 64
BLOCK_TILES = 48
CHUNK_TILES = 8
CHUNKS = BLOCK_TILES // CHUNK_TILES
ROWS = CHANNELS * CHUNK_TILES
SPOTS = 8
UNITS = (
    (0, 0, 1, 'P'),
    (0, 1, 2, 'P'),
    (0, 3, 1, 'P'),
    (1, 0, 1, 'P'),
    (1, 1, 2, 'P'),
    (1, 3, 1, 'P'),
    (2, 0, 2, 'P'),
    (2, 2, 2, 'T'),
    (3, 0, 1, 'T'),
    (3, 1, 2, 'T'),
    (3, 3, 1, 'T'),
    (4, 0, 4, 'T'),
    (5, 0, 1, 'T'),
    (5, 1, 1, 'T'),
    (5, 2, 1, 'T'),
    (5, 3, 1, 'T'),
)
LOADS = (0, 14, 7, 2, 11, 9, 8, 10, 1, 12, 4, 5, 13, 3, 15, 6)
FAR = (5,)
PLAN = (
    ('L', 0), ('L', 14), ('L', 7), ('L', 2), ('L', 11), ('C', 0), ('S', 0), ('C', 14), ('S', 14),
    ('L', 9), ('C', 7), ('S', 7), ('C', 2), ('S', 2), ('L', 8), ('L', 10), ('L', 1), ('C', 11),
    ('S', 11), ('C', 9), ('L', 12), ('C', 8), ('L', 4), ('C', 10), ('L', 5), ('C', 1), ('S', 1),
    ('S', 9), ('A', 0), ('A', 14), ('L', 13), ('C', 12), ('L', 3), ('L', 15), ('L', 6), ('C', 4),
    ('S', 4), ('C', 5), ('C', 13), ('A', 2), ('C', 3), ('S', 5), ('C', 15), ('C', 6), ('A', 7),
    ('S', 3), ('S', 8), ('A', 1), ('B', 14), ('S', 6), ('S', 10), ('A', 4), ('A', 11), ('A', 5),
    ('B', 7), ('S', 12), ('A', 3), ('A', 9), ('D', 14), ('B', 0), ('S', 13), ('B', 2), ('S', 15),
    ('A', 8), ('A', 6), ('B', 11), ('B', 1), ('D', 7), ('A', 10), ('B', 9), ('B', 8), ('B', 4),
    ('B', 5), ('A', 12), ('D', 11), ('B', 10), ('G', 0), ('B', 3), ('A', 13), ('D', 9), ('D', 8),
    ('B', 12), ('A', 15), ('D', 10), ('B', 13), ('B', 6), ('D', 12), ('B', 15), ('D', 13), ('G', 4),
    ('G', 1), ('D', 15), ('G', 3), ('G', 2), ('F', 0), ('F', 4), ('F', 1), ('F', 3), ('F', 5),
    ('F', 2),
)


def spot_of(y, x):
    return 2 * y + x


def place_of(spot):
    return spot // 2, spot % 2


def over(a, b, a_front, b_front):
    through_a = 1.0 - b_front * b[3]
    through_b = 1.0 - a_front * a[3]
    return [through_a * a[ch] + through_b * b[ch] for ch in range(CHANNELS)]


def kernel(layers, mask_in, depth_in, out,
           inb, local, from_core, chip, from_pair, pair, from_cross, from_skip, gap, from_gap,
           merged, from_merged, quad, gathered, group, from_group, outv, tile_mask, depth,
           in_sem, core_recv, first_recv, second_recv, third_recv, plane_recv, group_recv, sent,
           small_sem):
    tri = lax.axis_index("tri")
    blk = lax.axis_index("blk")
    core = blk % 2
    z = (blk // 2) % 4
    x = (blk // 8) % 2
    y = blk // 16
    spot = spot_of(y, x)
    me = tri * BLOCKS + blk
    half = (z % 2 + z // 2) % 2
    item = z // 2

    def device(t, yy, xx, zz, cc):
        return (t, yy * 16 + xx * 8 + zz * 2 + cc)

    core_peer = device(tri, y, x, z, 1 - core)
    pair_peer = device(tri, y, x, z + 1 - 2 * (z % 2), core)
    cross_peer = device(tri, y, x, 3 - z, core)
    skew_peer = device(tri, y, x, (z + 2) % 4, core)
    tri_peer = device(1 - tri, y, x, z, core)

    def load_copy(u, m):
        k, first, _, _ = UNITS[u]
        return pltpu.make_async_copy(
            layers.at[:, m, :, :, pl.ds(ROWS * k, ROWS), :], inb.at[k, m], in_sem.at[u])

    def load_wait(u):
        k, first, count, _ = UNITS[u]
        pltpu.make_async_copy(
            inb.at[k, pl.ds(first, count)], inb.at[k, pl.ds(first, count)], in_sem.at[u]).wait()

    def load_start(u):
        k, first, count, _ = UNITS[u]
        for m in range(first, first + count):
            load_copy(u, m).start()

    def spots(u):
        k, first, count, _ = UNITS[u]
        return k, pl.ds(2 * first, 2 * count)

    def core_copy(u):
        k, part = spots(u)
        return pltpu.make_async_remote_copy(
            src_ref=local.at[k, 1 - core, :, :, part], dst_ref=from_core.at[k, :, :, part],
            send_sem=sent.at[0], recv_sem=core_recv.at[u],
            device_id=core_peer, device_id_type=MESH)

    def remote(src, dst, send_sem, recv_sem, peer):
        return pltpu.make_async_remote_copy(
            src_ref=src, dst_ref=dst, send_sem=send_sem, recv_sem=recv_sem,
            device_id=peer, device_id_type=MESH)

    def first_copy(u):
        k, part = spots(u)
        if UNITS[u][3] == "P":
            return remote(chip.at[k, 1 - half, :, part], from_pair.at[k, :, part],
                          sent.at[1], first_recv.at[u], pair_peer)
        return remote(chip.at[k, :, 1 - item, part], from_skip.at[k, :, part],
                      sent.at[1], first_recv.at[u], cross_peer)

    def flat(u):
        k, first, count, _ = UNITS[u]
        return pl.ds(SPOTS * k + 2 * first, 2 * count)

    def second_copy(u):
        k, part = spots(u)
        if UNITS[u][3] == "P":
            return remote(pair.at[k, 1 - item, part], from_cross.at[flat(u)],
                          sent.at[2], second_recv.at[u], cross_peer)
        return remote(gap.at[flat(u)], from_gap.at[flat(u)],
                      sent.at[3], second_recv.at[u], pair_peer)

    def third_copy(u):
        return remote(merged.at[flat(u)], from_merged.at[flat(u)],
                      sent.at[4], third_recv.at[u], pair_peer)

    def group_copy(k):
        return remote(group.at[k], from_group.at[k], sent.at[5], group_recv.at[k], tri_peer)

    def all_sent():
        plain = sum(2 * unit[2] for unit in UNITS if unit[3] == "P")
        skip = sum(2 * unit[2] for unit in UNITS if unit[3] == "T")
        near = CHUNKS - len(FAR)
        plane_copies = near * (SPOTS - 1) + len(FAR) * (2 * SPOTS - 1)
        for n, ref in enumerate((
                from_core, from_skip, from_cross.at[pl.ds(0, plain)], from_gap.at[pl.ds(0, skip)],
                from_merged.at[pl.ds(0, skip)], group.at[pl.ds(0, near)],
                gathered.at[pl.ds(0, plane_copies)])):
            remote(ref, ref, sent.at[n], core_recv.at[0], core_peer).wait_send()

    def plane_copy(k, t, other):
        yy, xx = place_of(other)
        return pltpu.make_async_remote_copy(
            src_ref=quad.at[k, other], dst_ref=gathered.at[2 * SPOTS * k + tri * SPOTS + spot],
            send_sem=sent.at[6], recv_sem=plane_recv.at[k],
            device_id=device(t, yy, xx, z, core), device_id_type=MESH)

    def plane_all(k):
        count = 2 * SPOTS - 1 if k in FAR else SPOTS - 1
        return remote(gathered.at[pl.ds(0, count)], gathered.at[pl.ds(0, count)],
                      sent.at[6], plane_recv.at[k], core_peer)

    mask_copy = pltpu.make_async_copy(mask_in, tile_mask, small_sem.at[0])
    depth_copy = pltpu.make_async_copy(depth_in, depth, small_sem.at[1])
    mask_copy.start()
    depth_copy.start()
    for u in LOADS[:2]:
        load_start(u)

    barrier = pltpu.get_barrier_semaphore()
    for peer in (core_peer, pair_peer, cross_peer):
        pl.semaphore_signal(barrier, inc=1, device_id=peer, device_id_type=MESH)
    for step in range(1, 2 * SPOTS):
        t = (tri + step // SPOTS) % 2
        yy, xx = place_of((spot + step) % SPOTS)
        pl.semaphore_signal(barrier, inc=1, device_id=device(t, yy, xx, z, core), device_id_type=MESH)

    for u in LOADS[2:]:
        load_start(u)
    mask_copy.wait()
    depth_copy.wait()

    def nearer(left, right):
        return jnp.where(
            depth[RANK_DEV * left] < depth[RANK_DEV * right], 1.0, 0.0).astype(jnp.float32)

    own = [depth[RANK_DEV * me + r] for r in range(RANK_DEV)]
    front = [[jnp.where(own[j] < own[r], 1.0, 0.0).astype(jnp.float32) for r in range(RANK_DEV)]
             for j in range(RANK_DEV)]

    def number(peer):
        return peer[0] * BLOCKS + peer[1]

    def flags(peer):
        return nearer(me, number(peer)), nearer(number(peer), me)

    core_flags = flags(core_peer)
    pair_flags = flags(pair_peer)
    cross_flags = flags(cross_peer)
    group_flags = flags(tri_peer)

    chips = {"w": me, "v": number(cross_peer), "p": number(pair_peer), "q": number(skew_peer)}
    f = {a + b: nearer(chips[a], chips[b]) for a in chips for b in chips if a != b}
    w_between = f["pw"] * f["wq"] + f["qw"] * f["wp"]
    v_between = f["pv"] * f["vq"] + f["qv"] * f["vp"]
    w_ahead = f["wp"] * f["wq"]
    v_ahead = f["vp"] * f["vq"]

    def quad_device(q):
        return (q // 8) * BLOCKS + (q // 2) % 4 * 16 + q % 2 * 8

    def tree_flags(leaves, base):
        levels = []
        span = 1
        while span < leaves:
            levels.append([
                (nearer(base + quad_device(q), base + quad_device(q + span)),
                 nearer(base + quad_device(q + span), base + quad_device(q)))
                for q in range(0, leaves, 2 * span)])
            span *= 2
        return levels

    far_flags = tree_flags(2 * SPOTS, 0) if FAR else None
    near_flags = tree_flags(SPOTS, tri * BLOCKS)

    sub = lax.broadcasted_iota(jnp.int32, (CHUNK_TILES, 128), 0)

    def mask_of(r, group):
        value = jnp.zeros((CHUNK_TILES, 128), jnp.float32)
        for s in range(CHUNK_TILES):
            on = tile_mask[r, 0, CHUNK_TILES * group + s].astype(jnp.float32)
            value = jnp.where(sub == s, on, value)
        return value

    masks = [[mask_of(r, g) for r in range(RANK_DEV)] for g in range(COLUMN_TILES // CHUNK_TILES)]

    def span_of(u):
        k, first, count, _ = UNITS[u]
        return 2 * first, 2 * (first + count)

    def blend_local(u, to_core):
        k = UNITS[u][0]
        mask = masks[k % (COLUMN_TILES // CHUNK_TILES)]
        @pl.loop(*span_of(u))
        def _(o):
            for hh, ii in ((0, 0), (0, 1), (1, 0), (1, 1)):
                block = (hh + ii * (3 - 2 * hh)) * 2 + to_core

                def plane(r, ch):
                    return inb[k, o // 2, r, o % 2, block,
                               pl.ds(ch, CHUNK_TILES, stride=CHANNELS), :]

                opacity = [mask[r] * plane(r, 3) for r in range(RANK_DEV)]
                weights = []
                for r in range(RANK_DEV):
                    weight = mask[r]
                    for j in range(RANK_DEV):
                        if j != r:
                            weight = weight * (1.0 - front[j][r] * opacity[j])
                    weights.append(weight)
                for ch in range(CHANNELS):
                    total = weights[0] * plane(0, ch)
                    for r in range(1, RANK_DEV):
                        total = total + weights[r] * plane(r, ch)
                    local[k, to_core, hh, ii, o, ch] = total

    def planes(ref, *index):
        return [ref[index + (ch,)] for ch in range(CHANNELS)]

    def blend_chip(u, sent):
        k, _, _, kind = UNITS[u]

        @pl.loop(*span_of(u))
        def _(o):
            for n in range(2):
                if kind == "P":
                    hh, ii = 1 - half if sent else half, n
                else:
                    hh, ii = n, 1 - item if sent else item
                a = planes(local, k, core, hh, ii, o)
                b = planes(from_core, k, hh, ii, o)
                for ch, value in enumerate(over(a, b, *core_flags)):
                    chip[k, hh, ii, o, ch] = value

    def blend_pair(u, to_item):
        k = UNITS[u][0]

        @pl.loop(*span_of(u), unroll=2)
        def _(o):
            a = planes(chip, k, half, to_item, o)
            b = planes(from_pair, k, to_item, o)
            for ch, value in enumerate(over(a, b, *pair_flags)):
                pair[k, to_item, o, ch] = value

    def blend_cross(u):
        k = UNITS[u][0]

        @pl.loop(*span_of(u), unroll=2)
        def _(o):
            a = planes(pair, k, item, o)
            b = planes(from_cross, SPOTS * k + o)
            for ch, value in enumerate(over(a, b, *cross_flags)):
                quad[k, o, ch] = value

    def blend_gap(u):
        k = UNITS[u][0]

        @pl.loop(*span_of(u), unroll=2)
        def _(o):
            gap[SPOTS * k + o] = ((1.0 - w_between * chip[k, half, item, o, 3])
                         * (1.0 - v_between * from_skip[k, half, o, 3]))

    def blend_merged(u):
        k = UNITS[u][0]

        @pl.loop(*span_of(u), unroll=2)
        def _(o):
            w = planes(chip, k, 1 - half, item, o)
            v = planes(from_skip, k, 1 - half, o)
            g = from_gap[SPOTS * k + o]
            weight_w = f["wv"] + f["vw"] * ((1.0 - v[3]) * g)
            weight_v = f["vw"] + f["wv"] * ((1.0 - w[3]) * g)
            for ch in range(3):
                merged[SPOTS * k + o, ch] = weight_w * w[ch] + weight_v * v[ch]
            merged[SPOTS * k + o, 3] = w[3]
            merged[SPOTS * k + o, 4] = v[3]

    def blend_skip(u):
        k = UNITS[u][0]

        @pl.loop(*span_of(u), unroll=2)
        def _(o):
            w = planes(chip, k, half, item, o)
            v = planes(from_skip, k, half, o)
            g = gap[SPOTS * k + o]
            p = from_merged[SPOTS * k + o, 3]
            q = from_merged[SPOTS * k + o, 4]
            m = [from_merged[SPOTS * k + o, ch] for ch in range(3)]
            m.append((f["pq"] + f["qp"] * ((1.0 - q) * g)) * p
                     + (f["qp"] + f["pq"] * ((1.0 - p) * g)) * q)
            weight_w = (1.0 - f["vw"] * v[3]) * (1.0 - f["pw"] * p) * (1.0 - f["qw"] * q)
            weight_v = (1.0 - f["wv"] * w[3]) * (1.0 - f["pv"] * p) * (1.0 - f["qv"] * q)
            weight_m = (1.0 - w_ahead * w[3]) * (1.0 - v_ahead * v[3])
            for ch in range(CHANNELS):
                quad[k, o, ch] = weight_w * w[ch] + weight_v * v[ch] + weight_m * m[ch]

    def blend_tree(k, leaves, base, levels):
        for ch in range(CHANNELS):
            gathered[2 * SPOTS * k + tri * SPOTS + spot, ch] = quad[k, spot, ch]
        images = []
        for q in range(leaves):
            slot = 2 * SPOTS * k + base + (q // SPOTS) * SPOTS + spot_of((q // 2) % 4, q % 2)
            images.append(planes(gathered, slot))
        for level in levels:
            images = [over(images[2 * n], images[2 * n + 1], *level[n]) for n in range(len(level))]
        return images[0]

    def put(k, image):
        for ch in range(CHANNELS):
            outv[pl.ds(ROWS * k + ch, CHUNK_TILES, stride=CHANNELS), :] = image[ch]

    def stage_load(u):
        with jax.named_scope(f"L_wait{u}"):
            load_wait(u)
        with jax.named_scope(f"L_send{u}"):
            blend_local(u, 1 - core)
        if u == LOADS[0]:
            with jax.named_scope("w_barrier"):
                pl.semaphore_wait(barrier, 18)
        core_copy(u).start()
        with jax.named_scope(f"L_own{u}"):
            blend_local(u, core)

    def stage_chip(u):
        with jax.named_scope(f"C_wait{u}"):
            core_copy(u).wait_recv()
        with jax.named_scope(f"C_run{u}"):
            blend_chip(u, True)

    def stage_send(u):
        first_copy(u).start()
        with jax.named_scope(f"S_run{u}"):
            blend_chip(u, False)

    def stage_first(u):
        with jax.named_scope(f"A_wait{u}"):
            first_copy(u).wait_recv()
        if UNITS[u][3] == "P":
            with jax.named_scope(f"A_run{u}"):
                blend_pair(u, 1 - item)
            second_copy(u).start()
            blend_pair(u, item)
        else:
            with jax.named_scope(f"A_run{u}"):
                blend_gap(u)
            second_copy(u).start()

    def send_planes(u):
        k, first, count, _ = UNITS[u]
        for step in range(4 * count if k in FAR else 2 * count):
            other = 2 * first + (spot + step) % (2 * count)
            t = (tri + 1 + step // (2 * count)) % 2 if k in FAR else tri

            @pl.when((t != tri) | (other != spot))
            def _():
                plane_copy(k, t, other).start()

    def stage_second(u):
        with jax.named_scope(f"B_wait{u}"):
            second_copy(u).wait_recv()
        if UNITS[u][3] == "P":
            with jax.named_scope(f"B_run{u}"):
                blend_cross(u)
                send_planes(u)
        else:
            with jax.named_scope(f"B_run{u}"):
                blend_merged(u)
            third_copy(u).start()

    def stage_third(u):
        with jax.named_scope(f"D_wait{u}"):
            third_copy(u).wait_recv()
        with jax.named_scope(f"D_run{u}"):
            blend_skip(u)
            send_planes(u)

    def stage_group(k):
        with jax.named_scope(f"G_wait{k}"):
            plane_all(k).wait_recv()
        with jax.named_scope(f"G_run{k}"):
            for ch, value in enumerate(blend_tree(k, SPOTS, tri * SPOTS, near_flags)):
                group[k, ch] = value
        group_copy(k).start()

    def stage_out(k):
        if k in FAR:
            with jax.named_scope(f"F_wait{k}"):
                plane_all(k).wait_recv()
            with jax.named_scope(f"F_run{k}"):
                put(k, blend_tree(k, 2 * SPOTS, 0, far_flags))
        else:
            with jax.named_scope(f"F_wait{k}"):
                group_copy(k).wait_recv()
            with jax.named_scope(f"F_run{k}"):
                put(k, over(planes(group, k), planes(from_group, k), *group_flags))

    stages = {"L": stage_load, "C": stage_chip, "S": stage_send, "A": stage_first,
              "B": stage_second, "D": stage_third, "G": stage_group, "F": stage_out}
    for name, which in PLAN:
        stages[name](which)
    with jax.named_scope("w_sends"):
        all_sent()
    with jax.named_scope("w_out"):
        result = pltpu.make_async_copy(outv, out, small_sem.at[0])
        result.start()
        result.wait()


def on_device(layers, tile_mask, depth_order):
    rank_dev, channels, pixels = layers.shape
    tiles = pixels // 128
    rows = layers.reshape(rank_dev, channels, tiles, 128).transpose(0, 2, 1, 3)
    rows = rows.reshape(rank_dev, 4, 2, 8, BLOCK_TILES * channels, 128)
    plane = (CHUNK_TILES, 128)
    image = (CHANNELS,) + plane
    units = len(UNITS)
    dma = pltpu.SemaphoreType.DMA
    out = pl.pallas_call(
        kernel,
        out_shape=jax.ShapeDtypeStruct((BLOCK_TILES * channels, 128), jnp.float32),
        in_specs=[pl.BlockSpec(memory_space=pltpu.HBM)] * 3,
        out_specs=pl.BlockSpec(memory_space=pl.ANY),
        scratch_shapes=[
            pltpu.VMEM((CHUNKS, 4, rank_dev, 2, 8, ROWS, 128), jnp.float32),
            pltpu.VMEM((CHUNKS, 2, 2, 2, SPOTS) + image, jnp.float32),
            pltpu.VMEM((CHUNKS, 2, 2, SPOTS) + image, jnp.float32),
            pltpu.VMEM((CHUNKS, 2, 2, SPOTS) + image, jnp.float32),
            pltpu.VMEM((CHUNKS, 2, SPOTS) + image, jnp.float32),
            pltpu.VMEM((CHUNKS, 2, SPOTS) + image, jnp.float32),
            pltpu.VMEM((CHUNKS * SPOTS,) + image, jnp.float32),
            pltpu.VMEM((CHUNKS, 2, SPOTS) + image, jnp.float32),
            pltpu.VMEM((CHUNKS * SPOTS,) + plane, jnp.float32),
            pltpu.VMEM((CHUNKS * SPOTS,) + plane, jnp.float32),
            pltpu.VMEM((CHUNKS * SPOTS, 5) + plane, jnp.float32),
            pltpu.VMEM((CHUNKS * SPOTS, 5) + plane, jnp.float32),
            pltpu.VMEM((CHUNKS, SPOTS) + image, jnp.float32),
            pltpu.VMEM((CHUNKS * 2 * SPOTS,) + image, jnp.float32),
            pltpu.VMEM((CHUNKS,) + image, jnp.float32),
            pltpu.VMEM((CHUNKS,) + image, jnp.float32),
            pltpu.VMEM((BLOCK_TILES * channels, 128), jnp.float32),
            pltpu.SMEM(tile_mask.shape, jnp.int32),
            pltpu.SMEM(depth_order.shape, jnp.int32),
            dma((units,)), dma((units,)), dma((units,)), dma((units,)), dma((units,)),
            dma((CHUNKS,)), dma((CHUNKS,)), dma((7,)),
            dma((2,)),
        ],
        compiler_params=pltpu.CompilerParams(
            collective_id=0, has_side_effects=True, vmem_limit_bytes=60 * 1024 * 1024),
    )(rows, tile_mask, depth_order)
    out = out.reshape(BLOCK_TILES, channels, 128).transpose(1, 0, 2)
    return out.reshape(channels, BLOCK_TILES * 128)


def solution(mesh):
    in_specs = (P(("tri", "blk"), None, None), P(("tri", "blk"), None, None), P())
    out_specs = P(None, "blk")
    return jax.shard_map(
        on_device, mesh=mesh, in_specs=in_specs, out_specs=out_specs, check_vma=False
    )
```

```python
import jax
import jax.numpy as jnp
from jax import lax
from jax.experimental import pallas as pl
from jax.experimental.pallas import tpu as pltpu
from jax.sharding import PartitionSpec as P

MESH = pl.DeviceIdType.MESH
RANK_DEV = 3
CHANNELS = 4
COLUMN_TILES = 24
BLOCKS = 64
BLOCK_TILES = 48
CHUNK_TILES = 8
CHUNKS = BLOCK_TILES // CHUNK_TILES
ROWS = CHANNELS * CHUNK_TILES
SPOTS = 8
UNITS = (
    (0, 0, 1, 'P'),
    (0, 1, 1, 'P'),
    (0, 2, 1, 'P'),
    (0, 3, 1, 'P'),
    (1, 0, 4, 'P'),
    (2, 0, 1, 'P'),
    (2, 1, 1, 'P'),
    (2, 2, 1, 'T'),
    (2, 3, 1, 'T'),
    (3, 0, 2, 'T'),
    (3, 2, 1, 'T'),
    (3, 3, 1, 'T'),
    (4, 0, 2, 'T'),
    (4, 2, 2, 'T'),
    (5, 0, 1, 'T'),
    (5, 1, 1, 'T'),
    (5, 2, 1, 'T'),
    (5, 3, 1, 'T'),
)
LOADS = (7, 1, 8, 4, 12, 2, 5, 9, 6, 14, 0, 13, 11, 3, 10, 16, 15, 17)
FAR = (2, 4, 5)
PLAN = (
    ('L', 7), ('L', 1), ('L', 8), ('L', 4), ('C', 7), ('S', 7), ('L', 12), ('C', 1), ('S', 1),
    ('C', 8), ('S', 8), ('L', 2), ('L', 5), ('L', 9), ('C', 4), ('L', 6), ('S', 4), ('C', 12),
    ('S', 12), ('C', 2), ('C', 5), ('L', 14), ('L', 0), ('L', 13), ('C', 9), ('S', 9), ('C', 6),
    ('L', 11), ('A', 7), ('L', 3), ('C', 14), ('L', 10), ('A', 1), ('C', 0), ('L', 16), ('L', 15),
    ('C', 13), ('L', 17), ('C', 11), ('A', 8), ('C', 3), ('C', 10), ('C', 16), ('C', 15), ('C', 17),
    ('S', 14), ('A', 12), ('S', 13), ('S', 2), ('A', 4), ('B', 7), ('B', 8), ('B', 12), ('A', 9),
    ('B', 1), ('A', 2), ('D', 7), ('A', 14), ('D', 8), ('S', 5), ('S', 11), ('D', 12), ('S', 6),
    ('A', 13), ('B', 9), ('S', 10), ('B', 14), ('S', 16), ('A', 5), ('B', 4), ('A', 6), ('B', 13),
    ('B', 2), ('S', 15), ('A', 11), ('D', 9), ('S', 17), ('D', 14), ('S', 0), ('A', 10), ('S', 3),
    ('A', 16), ('D', 13), ('B', 11), ('B', 5), ('B', 6), ('A', 0), ('G', 1), ('B', 10), ('A', 15),
    ('A', 3), ('B', 16), ('A', 17), ('D', 11), ('B', 0), ('D', 10), ('B', 15), ('B', 3), ('D', 16),
    ('B', 17), ('D', 15), ('G', 3), ('D', 17), ('G', 0), ('F', 1), ('F', 4), ('F', 2), ('F', 3),
    ('F', 5), ('F', 0),
)


def spot_of(y, x):
    return 2 * y + x


def place_of(spot):
    return spot // 2, spot % 2


def over(a, b, a_front, b_front):
    through_a = 1.0 - b_front * b[3]
    through_b = 1.0 - a_front * a[3]
    return [through_a * a[ch] + through_b * b[ch] for ch in range(CHANNELS)]


def kernel(layers, mask_in, depth_in, out,
           inb, local, from_core, chip, from_pair, pair, from_cross, from_skip, gap, from_gap,
           merged, from_merged, quad, gathered, group, from_group, tile_mask, depth,
           in_sem, core_recv, first_recv, second_recv, third_recv, plane_recv, group_recv, sent,
           small_sem):
    tri = lax.axis_index("tri")
    blk = lax.axis_index("blk")
    core = blk % 2
    z = (blk // 2) % 4
    x = (blk // 8) % 2
    y = blk // 16
    spot = spot_of(y, x)
    me = tri * BLOCKS + blk
    half = (z % 2 + z // 2) % 2
    item = z // 2

    def device(t, yy, xx, zz, cc):
        return (t, yy * 16 + xx * 8 + zz * 2 + cc)

    core_peer = device(tri, y, x, z, 1 - core)
    pair_peer = device(tri, y, x, z + 1 - 2 * (z % 2), core)
    cross_peer = device(tri, y, x, 3 - z, core)
    skew_peer = device(tri, y, x, (z + 2) % 4, core)
    tri_peer = device(1 - tri, y, x, z, core)

    def load_copy(u, m):
        k, first, _, _ = UNITS[u]
        return pltpu.make_async_copy(
            layers.at[:, m, :, :, pl.ds(ROWS * k, ROWS), :], inb.at[k, m], in_sem.at[u])

    def load_wait(u):
        k, first, count, _ = UNITS[u]
        pltpu.make_async_copy(
            inb.at[k, pl.ds(first, count)], inb.at[k, pl.ds(first, count)], in_sem.at[u]).wait()

    def load_start(u):
        k, first, count, _ = UNITS[u]
        for m in range(first, first + count):
            load_copy(u, m).start()

    def spots(u):
        k, first, count, _ = UNITS[u]
        return k, pl.ds(2 * first, 2 * count)

    def core_copy(u):
        k, part = spots(u)
        return pltpu.make_async_remote_copy(
            src_ref=local.at[k, 1 - core, :, :, part], dst_ref=from_core.at[k, :, :, part],
            send_sem=sent.at[0], recv_sem=core_recv.at[u],
            device_id=core_peer, device_id_type=MESH)

    def remote(src, dst, send_sem, recv_sem, peer):
        return pltpu.make_async_remote_copy(
            src_ref=src, dst_ref=dst, send_sem=send_sem, recv_sem=recv_sem,
            device_id=peer, device_id_type=MESH)

    def first_copy(u):
        k, part = spots(u)
        if UNITS[u][3] == "P":
            return remote(chip.at[k, 1 - half, :, part], from_pair.at[k, :, part],
                          sent.at[1], first_recv.at[u], pair_peer)
        return remote(chip.at[k, :, 1 - item, part], from_skip.at[k, :, part],
                      sent.at[1], first_recv.at[u], cross_peer)

    def flat(u):
        k, first, count, _ = UNITS[u]
        return pl.ds(SPOTS * k + 2 * first, 2 * count)

    def second_copy(u):
        k, part = spots(u)
        if UNITS[u][3] == "P":
            return remote(pair.at[k, 1 - item, part], from_cross.at[flat(u)],
                          sent.at[2], second_recv.at[u], cross_peer)
        return remote(gap.at[flat(u)], from_gap.at[flat(u)],
                      sent.at[3], second_recv.at[u], pair_peer)

    def third_copy(u):
        return remote(merged.at[flat(u)], from_merged.at[flat(u)],
                      sent.at[4], third_recv.at[u], pair_peer)

    def group_copy(k):
        return remote(group.at[k], from_group.at[k], sent.at[5], group_recv.at[k], tri_peer)

    def all_sent():
        plain = sum(2 * unit[2] for unit in UNITS if unit[3] == "P")
        skip = sum(2 * unit[2] for unit in UNITS if unit[3] == "T")
        near = CHUNKS - len(FAR)
        plane_copies = near * (SPOTS - 1) + len(FAR) * (2 * SPOTS - 1)
        for n, ref in enumerate((
                from_core, from_skip, from_cross.at[pl.ds(0, plain)], from_gap.at[pl.ds(0, skip)],
                from_merged.at[pl.ds(0, skip)], group.at[pl.ds(0, near)],
                gathered.at[pl.ds(0, plane_copies)])):
            remote(ref, ref, sent.at[n], core_recv.at[0], core_peer).wait_send()

    def plane_copy(k, t, other):
        yy, xx = place_of(other)
        return pltpu.make_async_remote_copy(
            src_ref=quad.at[k, other], dst_ref=gathered.at[2 * SPOTS * k + tri * SPOTS + spot],
            send_sem=sent.at[6], recv_sem=plane_recv.at[k],
            device_id=device(t, yy, xx, z, core), device_id_type=MESH)

    def plane_all(k):
        count = 2 * SPOTS - 1 if k in FAR else SPOTS - 1
        return remote(gathered.at[pl.ds(0, count)], gathered.at[pl.ds(0, count)],
                      sent.at[6], plane_recv.at[k], core_peer)

    mask_copy = pltpu.make_async_copy(mask_in, tile_mask, small_sem.at[0])
    depth_copy = pltpu.make_async_copy(depth_in, depth, small_sem.at[1])
    mask_copy.start()
    depth_copy.start()
    for u in LOADS[:2]:
        load_start(u)

    barrier = pltpu.get_barrier_semaphore()
    for peer in (core_peer, pair_peer, cross_peer):
        pl.semaphore_signal(barrier, inc=1, device_id=peer, device_id_type=MESH)
    for step in range(1, 2 * SPOTS):
        t = (tri + step // SPOTS) % 2
        yy, xx = place_of((spot + step) % SPOTS)
        pl.semaphore_signal(barrier, inc=1, device_id=device(t, yy, xx, z, core), device_id_type=MESH)

    for u in LOADS[2:]:
        load_start(u)
    mask_copy.wait()
    depth_copy.wait()

    def nearer(left, right):
        return jnp.where(
            depth[RANK_DEV * left] < depth[RANK_DEV * right], 1.0, 0.0).astype(jnp.float32)

    own = [depth[RANK_DEV * me + r] for r in range(RANK_DEV)]
    front = [[jnp.where(own[j] < own[r], 1.0, 0.0).astype(jnp.float32) for r in range(RANK_DEV)]
             for j in range(RANK_DEV)]

    def number(peer):
        return peer[0] * BLOCKS + peer[1]

    def flags(peer):
        return nearer(me, number(peer)), nearer(number(peer), me)

    core_flags = flags(core_peer)
    pair_flags = flags(pair_peer)
    cross_flags = flags(cross_peer)
    group_flags = flags(tri_peer)

    chips = {"w": me, "v": number(cross_peer), "p": number(pair_peer), "q": number(skew_peer)}
    f = {a + b: nearer(chips[a], chips[b]) for a in chips for b in chips if a != b}
    w_between = f["pw"] * f["wq"] + f["qw"] * f["wp"]
    v_between = f["pv"] * f["vq"] + f["qv"] * f["vp"]
    w_ahead = f["wp"] * f["wq"]
    v_ahead = f["vp"] * f["vq"]

    def quad_device(q):
        return (q // 8) * BLOCKS + (q // 2) % 4 * 16 + q % 2 * 8

    def tree_flags(leaves, base):
        levels = []
        span = 1
        while span < leaves:
            levels.append([
                (nearer(base + quad_device(q), base + quad_device(q + span)),
                 nearer(base + quad_device(q + span), base + quad_device(q)))
                for q in range(0, leaves, 2 * span)])
            span *= 2
        return levels

    far_flags = tree_flags(2 * SPOTS, 0) if FAR else None
    near_flags = tree_flags(SPOTS, tri * BLOCKS)

    sub = lax.broadcasted_iota(jnp.int32, (CHUNK_TILES, 128), 0)

    def mask_of(r, group):
        value = jnp.zeros((CHUNK_TILES, 128), jnp.float32)
        for s in range(CHUNK_TILES):
            on = tile_mask[r, 0, CHUNK_TILES * group + s].astype(jnp.float32)
            value = jnp.where(sub == s, on, value)
        return value

    masks = [[mask_of(r, g) for r in range(RANK_DEV)] for g in range(COLUMN_TILES // CHUNK_TILES)]

    def span_of(u):
        k, first, count, _ = UNITS[u]
        return 2 * first, 2 * (first + count)

    def blend_local(u, to_core):
        k = UNITS[u][0]
        mask = masks[k % (COLUMN_TILES // CHUNK_TILES)]
        @pl.loop(*span_of(u))
        def _(o):
            for hh, ii in ((0, 0), (0, 1), (1, 0), (1, 1)):
                block = (hh + ii * (3 - 2 * hh)) * 2 + to_core

                def plane(r, ch):
                    return inb[k, o // 2, r, o % 2, block,
                               pl.ds(ch, CHUNK_TILES, stride=CHANNELS), :]

                opacity = [mask[r] * plane(r, 3) for r in range(RANK_DEV)]
                weights = []
                for r in range(RANK_DEV):
                    weight = mask[r]
                    for j in range(RANK_DEV):
                        if j != r:
                            weight = weight * (1.0 - front[j][r] * opacity[j])
                    weights.append(weight)
                for ch in range(CHANNELS):
                    total = weights[0] * plane(0, ch)
                    for r in range(1, RANK_DEV):
                        total = total + weights[r] * plane(r, ch)
                    local[k, to_core, hh, ii, o, ch] = total

    def planes(ref, *index):
        return [ref[index + (ch,)] for ch in range(CHANNELS)]

    def blend_chip(u, sent):
        k, _, _, kind = UNITS[u]

        @pl.loop(*span_of(u))
        def _(o):
            for n in range(2):
                if kind == "P":
                    hh, ii = 1 - half if sent else half, n
                else:
                    hh, ii = n, 1 - item if sent else item
                a = planes(local, k, core, hh, ii, o)
                b = planes(from_core, k, hh, ii, o)
                for ch, value in enumerate(over(a, b, *core_flags)):
                    chip[k, hh, ii, o, ch] = value

    def blend_pair(u, to_item):
        k = UNITS[u][0]

        @pl.loop(*span_of(u), unroll=2)
        def _(o):
            a = planes(chip, k, half, to_item, o)
            b = planes(from_pair, k, to_item, o)
            for ch, value in enumerate(over(a, b, *pair_flags)):
                pair[k, to_item, o, ch] = value

    def blend_cross(u):
        k = UNITS[u][0]

        @pl.loop(*span_of(u), unroll=2)
        def _(o):
            a = planes(pair, k, item, o)
            b = planes(from_cross, SPOTS * k + o)
            for ch, value in enumerate(over(a, b, *cross_flags)):
                quad[k, o, ch] = value

    def blend_gap(u):
        k = UNITS[u][0]

        @pl.loop(*span_of(u), unroll=2)
        def _(o):
            gap[SPOTS * k + o] = ((1.0 - w_between * chip[k, half, item, o, 3])
                         * (1.0 - v_between * from_skip[k, half, o, 3]))

    def blend_merged(u):
        k = UNITS[u][0]

        @pl.loop(*span_of(u), unroll=2)
        def _(o):
            w = planes(chip, k, 1 - half, item, o)
            v = planes(from_skip, k, 1 - half, o)
            g = from_gap[SPOTS * k + o]
            weight_w = f["wv"] + f["vw"] * ((1.0 - v[3]) * g)
            weight_v = f["vw"] + f["wv"] * ((1.0 - w[3]) * g)
            for ch in range(3):
                merged[SPOTS * k + o, ch] = weight_w * w[ch] + weight_v * v[ch]
            merged[SPOTS * k + o, 3] = w[3]
            merged[SPOTS * k + o, 4] = v[3]

    def blend_skip(u):
        k = UNITS[u][0]

        @pl.loop(*span_of(u), unroll=2)
        def _(o):
            w = planes(chip, k, half, item, o)
            v = planes(from_skip, k, half, o)
            g = gap[SPOTS * k + o]
            p = from_merged[SPOTS * k + o, 3]
            q = from_merged[SPOTS * k + o, 4]
            m = [from_merged[SPOTS * k + o, ch] for ch in range(3)]
            m.append((f["pq"] + f["qp"] * ((1.0 - q) * g)) * p
                     + (f["qp"] + f["pq"] * ((1.0 - p) * g)) * q)
            weight_w = (1.0 - f["vw"] * v[3]) * (1.0 - f["pw"] * p) * (1.0 - f["qw"] * q)
            weight_v = (1.0 - f["wv"] * w[3]) * (1.0 - f["pv"] * p) * (1.0 - f["qv"] * q)
            weight_m = (1.0 - w_ahead * w[3]) * (1.0 - v_ahead * v[3])
            for ch in range(CHANNELS):
                quad[k, o, ch] = weight_w * w[ch] + weight_v * v[ch] + weight_m * m[ch]

    def blend_tree(k, leaves, base, levels):
        for ch in range(CHANNELS):
            gathered[2 * SPOTS * k + tri * SPOTS + spot, ch] = quad[k, spot, ch]
        images = []
        for q in range(leaves):
            slot = 2 * SPOTS * k + base + (q // SPOTS) * SPOTS + spot_of((q // 2) % 4, q % 2)
            images.append(planes(gathered, slot))
        for level in levels:
            images = [over(images[2 * n], images[2 * n + 1], *level[n]) for n in range(len(level))]
        return images[0]

    def put(k, image):
        for ch in range(CHANNELS):
            out[pl.ds(ROWS * k + ch, CHUNK_TILES, stride=CHANNELS), :] = image[ch]

    def stage_load(u):
        with jax.named_scope(f"L_wait{u}"):
            load_wait(u)
        with jax.named_scope(f"L_send{u}"):
            blend_local(u, 1 - core)
        if u == LOADS[0]:
            with jax.named_scope("w_barrier"):
                pl.semaphore_wait(barrier, 18)
        core_copy(u).start()
        with jax.named_scope(f"L_own{u}"):
            blend_local(u, core)

    def stage_chip(u):
        with jax.named_scope(f"C_wait{u}"):
            core_copy(u).wait_recv()
        with jax.named_scope(f"C_run{u}"):
            blend_chip(u, True)

    def stage_send(u):
        first_copy(u).start()
        with jax.named_scope(f"S_run{u}"):
            blend_chip(u, False)

    def stage_first(u):
        with jax.named_scope(f"A_wait{u}"):
            first_copy(u).wait_recv()
        if UNITS[u][3] == "P":
            with jax.named_scope(f"A_run{u}"):
                blend_pair(u, 1 - item)
            second_copy(u).start()
            blend_pair(u, item)
        else:
            with jax.named_scope(f"A_run{u}"):
                blend_gap(u)
            second_copy(u).start()

    def send_planes(u):
        k, first, count, _ = UNITS[u]
        for step in range(4 * count if k in FAR else 2 * count):
            other = 2 * first + (spot + step) % (2 * count)
            t = (tri + 1 + step // (2 * count)) % 2 if k in FAR else tri

            @pl.when((t != tri) | (other != spot))
            def _():
                plane_copy(k, t, other).start()

    def stage_second(u):
        with jax.named_scope(f"B_wait{u}"):
            second_copy(u).wait_recv()
        if UNITS[u][3] == "P":
            with jax.named_scope(f"B_run{u}"):
                blend_cross(u)
                send_planes(u)
        else:
            with jax.named_scope(f"B_run{u}"):
                blend_merged(u)
            third_copy(u).start()

    def stage_third(u):
        with jax.named_scope(f"D_wait{u}"):
            third_copy(u).wait_recv()
        with jax.named_scope(f"D_run{u}"):
            blend_skip(u)
            send_planes(u)

    def stage_group(k):
        with jax.named_scope(f"G_wait{k}"):
            plane_all(k).wait_recv()
        with jax.named_scope(f"G_run{k}"):
            for ch, value in enumerate(blend_tree(k, SPOTS, tri * SPOTS, near_flags)):
                group[k, ch] = value
        group_copy(k).start()

    def stage_out(k):
        if k in FAR:
            with jax.named_scope(f"F_wait{k}"):
                plane_all(k).wait_recv()
            with jax.named_scope(f"F_run{k}"):
                put(k, blend_tree(k, 2 * SPOTS, 0, far_flags))
        else:
            with jax.named_scope(f"F_wait{k}"):
                group_copy(k).wait_recv()
            with jax.named_scope(f"F_run{k}"):
                put(k, over(planes(group, k), planes(from_group, k), *group_flags))

    stages = {"L": stage_load, "C": stage_chip, "S": stage_send, "A": stage_first,
              "B": stage_second, "D": stage_third, "G": stage_group, "F": stage_out}
    for name, which in PLAN:
        stages[name](which)
    with jax.named_scope("w_sends"):
        all_sent()


def on_device(layers, tile_mask, depth_order):
    rank_dev, channels, pixels = layers.shape
    tiles = pixels // 128
    rows = layers.reshape(rank_dev, channels, tiles, 128).transpose(0, 2, 1, 3)
    rows = rows.reshape(rank_dev, 4, 2, 8, BLOCK_TILES * channels, 128)
    plane = (CHUNK_TILES, 128)
    image = (CHANNELS,) + plane
    units = len(UNITS)
    dma = pltpu.SemaphoreType.DMA
    out = pl.pallas_call(
        kernel,
        out_shape=jax.ShapeDtypeStruct((BLOCK_TILES * channels, 128), jnp.float32),
        in_specs=[pl.BlockSpec(memory_space=pltpu.HBM)] * 3,
        out_specs=pl.BlockSpec(memory_space=pltpu.VMEM),
        scratch_shapes=[
            pltpu.VMEM((CHUNKS, 4, rank_dev, 2, 8, ROWS, 128), jnp.float32),
            pltpu.VMEM((CHUNKS, 2, 2, 2, SPOTS) + image, jnp.float32),
            pltpu.VMEM((CHUNKS, 2, 2, SPOTS) + image, jnp.float32),
            pltpu.VMEM((CHUNKS, 2, 2, SPOTS) + image, jnp.float32),
            pltpu.VMEM((CHUNKS, 2, SPOTS) + image, jnp.float32),
            pltpu.VMEM((CHUNKS, 2, SPOTS) + image, jnp.float32),
            pltpu.VMEM((CHUNKS * SPOTS,) + image, jnp.float32),
            pltpu.VMEM((CHUNKS, 2, SPOTS) + image, jnp.float32),
            pltpu.VMEM((CHUNKS * SPOTS,) + plane, jnp.float32),
            pltpu.VMEM((CHUNKS * SPOTS,) + plane, jnp.float32),
            pltpu.VMEM((CHUNKS * SPOTS, 5) + plane, jnp.float32),
            pltpu.VMEM((CHUNKS * SPOTS, 5) + plane, jnp.float32),
            pltpu.VMEM((CHUNKS, SPOTS) + image, jnp.float32),
            pltpu.VMEM((CHUNKS * 2 * SPOTS,) + image, jnp.float32),
            pltpu.VMEM((CHUNKS,) + image, jnp.float32),
            pltpu.VMEM((CHUNKS,) + image, jnp.float32),
            pltpu.SMEM(tile_mask.shape, jnp.int32),
            pltpu.SMEM(depth_order.shape, jnp.int32),
            dma((units,)), dma((units,)), dma((units,)), dma((units,)), dma((units,)),
            dma((CHUNKS,)), dma((CHUNKS,)), dma((7,)),
            dma((2,)),
        ],
        compiler_params=pltpu.CompilerParams(
            collective_id=0, has_side_effects=True, vmem_limit_bytes=45 * 1024 * 1024),
    )(rows, tile_mask, depth_order)
    out = out.reshape(BLOCK_TILES, channels, 128).transpose(1, 0, 2)
    return out.reshape(channels, BLOCK_TILES * 128)


def solution(mesh):
    in_specs = (P(("tri", "blk"), None, None), P(("tri", "blk"), None, None), P())
    out_specs = P(None, "blk")
    return jax.shard_map(
        on_device, mesh=mesh, in_specs=in_specs, out_specs=out_specs, check_vma=False
    )
```
